32 devices in a mesh: dp: 2 (over x), seq: 8 (over z, y), mp: 2 (over core).
Axes of the slice: x: 2, y: 2, z: 4, core: 2. Of those that a mesh axis runs over, the one named last changes fastest.
Arguments:
- inputs: bfloat16 [2, 2, 1024, 2304], P(None, 'dp', 'seq'), may hold values from -6 to 6
- cotangent: bfloat16 [2, 2, 1024, 2304], P(None, 'dp', 'seq'), may hold values from -6 to 6
- pre_attention: float32 [2304], replicated, may hold values from 0.5 to 1.5
- post_attention: float32 [2304], replicated, may hold values from 0.5 to 1.5
- pre_feedforward: float32 [2304], replicated, may hold values from 0.5 to 1.5
- post_feedforward: float32 [2304], replicated, may hold values from 0.5 to 1.5
- query_weight: bfloat16 [2304, 2048], P(('dp', 'seq'), 'mp'), may hold values from -0.625 to 0.625
- key_matrix: bfloat16 [2304, 1024], P(('dp', 'seq'), 'mp'), may hold values from -0.125 to 0.125
- value_matrix: bfloat16 [2304, 1024], P(('dp', 'seq'), 'mp'), may hold values from -0.125 to 0.125
- output_weight: bfloat16 [2048, 2304], P('mp', ('dp', 'seq')), may hold values from -0.125 to 0.125
- gate_weight: bfloat16 [2304, 9216], P(('dp', 'seq'), 'mp'), may hold values from -0.125 to 0.125
- up_weight: bfloat16 [2304, 9216], P(('dp', 'seq'), 'mp'), may hold values from -0.125 to 0.125
- down_weight: bfloat16 [9216, 2304], P('mp', ('dp', 'seq')), may hold values from -0.0625 to 0.0625
- adapter_down: bfloat16 [8, 16, 22784], replicated, may hold values from -0.125 to 0.125
- adapter_up: bfloat16 [8, 16, 27136], replicated, may hold values from -0.75 to 0.75
- prefix_lengths: int32 [2, 2], P(None, 'dp'), may hold values from 102 to 512
- adapter_choice: int32 [2, 2, 7], P(None, 'dp'), may hold values from 0 to 7
Outputs:
- outputs: bfloat16 [2, 2, 1024, 2304], P(None, 'dp', 'seq')
- input_gradient: bfloat16 [2, 2, 1024, 2304], P(None, 'dp', 'seq')
- down_gradient: float32 [8, 16, 22784], P(None, None, ('dp', 'seq', 'mp'))
- up_gradient: float32 [8, 16, 27136], P(None, None, ('dp', 'seq', 'mp'))
The draws below stay inside these ranges and needn't reach their ends.
All inputs are finite; a program needn't handle non-finite values.
Results may differ from the reference program's by a relative error of at most 0.02.
The reference program's roundings to bfloat16 on the way count: a program that leaves them out, or rounds other values in their place, can miss the bound.
Values may be sent and summed in bfloat16 or wider, within the bound.
A program may use at most 384 MiB of HBM per device.

```python
import jax
import jax.numpy as jnp
from jax import lax

MODEL_WIDTH = 2304
QUERY_HEADS_COUNT = 8
KEY_VALUE_HEADS = 4
HEAD_SIZE = 256
FF = 9216
R = 16
NAD = 8
MB = 2
SEQS = 2
SEQUENCE_LENGTH = 1024
AIN = 22784
BOUT = 27136


def draw_query_weight(key, part):
    pick_key = jax.random.fold_in(key, 11)
    noise_key = jax.random.fold_in(key, 12)
    half_heads = QUERY_HEADS_COUNT // 2
    chosen = jax.random.randint(pick_key, (2,), 0, half_heads) + jnp.array([0, half_heads], dtype=jnp.int32)
    head_ids = jnp.arange(QUERY_HEADS_COUNT, dtype=jnp.int32)
    strong = jnp.any(head_ids[:, None] == chosen[None, :], axis=1)
    factor = jnp.where(strong, 5.0, 1.0).astype(jnp.float32)
    column_factor = jnp.repeat(factor, HEAD_SIZE)
    base = jnp.clip(jax.random.normal(noise_key, (MODEL_WIDTH, QUERY_HEADS_COUNT * HEAD_SIZE), jnp.float32), -6.0, 6.0)
    value_rows = base * column_factor[None, :] * MODEL_WIDTH ** (-0.5)
    return value_rows.astype(jnp.bfloat16)


def with_ends(drawn, key, smallest, top_value):
    place = [jax.random.randint(jax.random.fold_in(key, axis), (), 0, length) for axis, length in enumerate(drawn.shape)]
    longest = drawn.shape.index(max(drawn.shape))
    beside = place[:longest] + [(place[longest] + 1) % drawn.shape[longest]] + place[longest + 1:]
    return drawn.at[tuple(place)].set(smallest).at[tuple(beside)].set(top_value)


def shard_levels(own_key, dims, split, least, top_value):
    level = 1.0
    for axis_at, blocks in split:
        heights = jax.random.uniform(jax.random.fold_in(jax.random.fold_in(own_key, 6), axis_at), (blocks,), jnp.float32, least / len(split), top_value / len(split))
        level = level * jnp.repeat(jnp.exp(heights), dims[axis_at] // blocks).reshape((-1,) + (1,) * (len(dims) - 1 - axis_at))
    return level


def normal_values(rng, shape, scale, most, split=(), kind=jnp.bfloat16):
    loudness = shard_levels(rng, shape, split, -0.22, 0.18) if split else 1.0
    drawn = jax.random.normal(rng, shape, jnp.float32) * scale * loudness
    return jnp.minimum(jnp.maximum(drawn, -most), most).astype(kind)


def setup_inputs(seed: int = 0) -> dict:
    streams_of = jax.random.split(jax.random.key(seed), 18)
    return {
        "inputs": normal_values(streams_of[0], (MB, SEQS, SEQUENCE_LENGTH, MODEL_WIDTH), 1.0, 6.0, ((1, 2), (2, 8))),
        "cotangent": normal_values(streams_of[1], (MB, SEQS, SEQUENCE_LENGTH, MODEL_WIDTH), 1.0, 6.0, ((1, 2), (2, 8))),
        "pre_attention": jnp.clip(1.0 + 0.1 * jax.random.normal(streams_of[2], (MODEL_WIDTH,), jnp.float32), 0.5, 1.5),
        "post_attention": jnp.clip(1.0 + 0.1 * jax.random.normal(streams_of[3], (MODEL_WIDTH,), jnp.float32), 0.5, 1.5),
        "pre_feedforward": jnp.clip(1.0 + 0.1 * jax.random.normal(streams_of[4], (MODEL_WIDTH,), jnp.float32), 0.5, 1.5),
        "post_feedforward": jnp.clip(1.0 + 0.1 * jax.random.normal(streams_of[5], (MODEL_WIDTH,), jnp.float32), 0.5, 1.5),
        "query_weight": draw_query_weight(jax.random.fold_in(streams_of[17], 71), 0),
        "key_matrix": normal_values(streams_of[7], (MODEL_WIDTH, KEY_VALUE_HEADS * HEAD_SIZE), MODEL_WIDTH ** -0.5, 0.125, ((0, 16), (1, 2))),
        "value_matrix": normal_values(streams_of[8], (MODEL_WIDTH, KEY_VALUE_HEADS * HEAD_SIZE), MODEL_WIDTH ** -0.5, 0.125, ((0, 16), (1, 2))),
        "output_weight": normal_values(streams_of[9], (QUERY_HEADS_COUNT * HEAD_SIZE, MODEL_WIDTH), (QUERY_HEADS_COUNT * HEAD_SIZE) ** -0.5, 0.125, ((0, 2), (1, 16))),
        "gate_weight": normal_values(streams_of[10], (MODEL_WIDTH, FF), MODEL_WIDTH ** -0.5, 0.125, ((0, 16), (1, 2))),
        "up_weight": normal_values(streams_of[11], (MODEL_WIDTH, FF), MODEL_WIDTH ** -0.5, 0.125, ((0, 16), (1, 2))),
        "down_weight": normal_values(streams_of[12], (FF, MODEL_WIDTH), FF ** -0.5, 0.0625, ((0, 2), (1, 16))),
        "adapter_down": normal_values(streams_of[13], (NAD, R, AIN), MODEL_WIDTH ** -0.5, 0.125),
        "adapter_up": normal_values(streams_of[14], (NAD, R, BOUT), (4 * R) ** -0.5, 0.75),
        "prefix_lengths": with_ends(jax.random.randint(streams_of[15], (MB, SEQS), SEQUENCE_LENGTH // 10, SEQUENCE_LENGTH // 2 + 1), jax.random.fold_in(streams_of[15], 1), SEQUENCE_LENGTH // 10, (SEQUENCE_LENGTH // 2 + 1) - 1).astype(jnp.int32),
        "adapter_choice": with_ends(jax.random.randint(streams_of[16], (MB, SEQS, 7), 0, NAD), jax.random.fold_in(streams_of[16], 1), 0, NAD - 1).astype(jnp.int32),
    }


HIGH = lax.Precision.HIGHEST
EPSILON = 1e-06
SOFT_CAP = 50.0

@jax.custom_vjp
def lower_factor(v):
    return lax.optimization_barrier(v.astype(jnp.bfloat16)).astype(jnp.float32)

@jax.custom_vjp
def low_back(v):
    return v

def low_keep(v):
    return (lower_factor(v), None)

def low_pass(kept, grad):
    return (grad,)

def back_keep(v):
    return (v, None)

def back_low(kept, grad):
    return (lower_factor(grad),)
lower_factor.defvjp(low_keep, low_pass)
low_back.defvjp(back_keep, back_low)

def normalize(value, gain):
    return value * lax.rsqrt(lax.optimization_barrier(jnp.mean(value * value, axis=-1, keepdims=True)) + EPSILON) * gain

def angles(length):
    half = HEAD_SIZE // 2
    rates = 10000.0 ** (-(jnp.arange(half, dtype=jnp.float32) * 2.0) / HEAD_SIZE)
    turns = jnp.arange(length, dtype=jnp.int32).astype(jnp.float32)[:, None] * rates[None, :]
    return (jnp.cos(turns)[:, None, :], jnp.sin(turns)[:, None, :])

def apply_rotation(head_stack, cosine_table, sine_table):
    half = HEAD_SIZE // 2
    first = head_stack[..., :half]
    second = head_stack[..., half:]
    return jnp.concatenate([first * cosine_table - second * sine_table, second * cosine_table + first * sine_table], axis=-1)

def attend_tokens(rotated_query, rotated_keys, value_rows, prefix_length):
    token_block = min(512, SEQUENCE_LENGTH)
    head_groups = QUERY_HEADS_COUNT // KEY_VALUE_HEADS

    def one_block(start_index):
        query_tile_block = lax.dynamic_slice_in_dim(rotated_query, start_index, token_block, 0).reshape(token_block, KEY_VALUE_HEADS, head_groups, HEAD_SIZE)
        raw = low_back(jnp.einsum('tkgd,skd->kgts', query_tile_block, rotated_keys, precision=HIGH) * HEAD_SIZE ** (-0.5))
        capped = SOFT_CAP * jnp.tanh(raw / SOFT_CAP)
        query_pos = start_index + jnp.arange(token_block, dtype=jnp.int32)
        key_pos = jnp.arange(SEQUENCE_LENGTH, dtype=jnp.int32)
        visible = (key_pos[None, :] <= query_pos[:, None]) | (key_pos[None, :] < prefix_length)
        masked = jnp.where(visible, capped, -1e+30)
        top = lax.optimization_barrier(jnp.max(masked, axis=-1, keepdims=True))
        expo = jnp.exp(masked - top)
        prob = lower_factor(expo / lax.optimization_barrier(jnp.sum(expo, axis=-1, keepdims=True)))
        result = jnp.einsum('kgts,skd->tkgd', prob, value_rows, precision=HIGH)
        return result.reshape(token_block, QUERY_HEADS_COUNT * HEAD_SIZE)
    starts = jnp.arange(SEQUENCE_LENGTH // token_block, dtype=jnp.int32) * token_block
    pieces = lax.map(jax.checkpoint(one_block), starts)
    return pieces.reshape(SEQUENCE_LENGTH, QUERY_HEADS_COUNT * HEAD_SIZE)

def layer(source, down_table, up_table, weights, gains, prefix_length, picks):
    query_weight, key_matrix, value_matrix, output_weight, gate_weight, up_weight, down_weight = weights
    first_gain, second_gain, third_gain, fourth_gain = gains
    query_width = QUERY_HEADS_COUNT * HEAD_SIZE
    key_span_width = KEY_VALUE_HEADS * HEAD_SIZE
    cosine_table, sine_table = angles(SEQUENCE_LENGTH)

    def project(inputs_low, weight, slot, in_start, in_size, out_start, out_size):
        down_part = down_table[picks[slot]][:, in_start:in_start + in_size]
        up_part = up_table[picks[slot]][:, out_start:out_start + out_size]
        inner = lower_factor(jnp.dot(inputs_low, down_part.T, precision=HIGH, preferred_element_type=jnp.float32))
        main = jnp.dot(inputs_low, weight, precision=HIGH, preferred_element_type=jnp.float32)
        return main + jnp.dot(inner, up_part, precision=HIGH, preferred_element_type=jnp.float32)
    normed = lower_factor(normalize(source, first_gain))
    query = low_back(project(normed, query_weight, 0, 0, MODEL_WIDTH, 0, query_width))
    key_rows = low_back(project(normed, key_matrix, 1, MODEL_WIDTH, MODEL_WIDTH, query_width, key_span_width))
    value_rows = lower_factor(low_back(project(normed, value_matrix, 2, 2 * MODEL_WIDTH, MODEL_WIDTH, query_width + key_span_width, key_span_width)))
    rotated_query = lower_factor(apply_rotation(query.reshape(SEQUENCE_LENGTH, QUERY_HEADS_COUNT, HEAD_SIZE), cosine_table, sine_table))
    rotated_keys = lower_factor(apply_rotation(key_rows.reshape(SEQUENCE_LENGTH, KEY_VALUE_HEADS, HEAD_SIZE), cosine_table, sine_table))
    head_stack = attend_tokens(rotated_query, rotated_keys, value_rows.reshape(SEQUENCE_LENGTH, KEY_VALUE_HEADS, HEAD_SIZE), prefix_length)
    head_stack = lower_factor(low_back(head_stack))
    attention_out = low_back(project(head_stack, output_weight, 3, 3 * MODEL_WIDTH, query_width, query_width + 2 * key_span_width, MODEL_WIDTH))
    middle = source + normalize(attention_out, second_gain)
    normed_ffw = lower_factor(normalize(middle, third_gain))
    gate = low_back(project(normed_ffw, gate_weight, 4, 3 * MODEL_WIDTH + query_width, MODEL_WIDTH, query_width + 2 * key_span_width + MODEL_WIDTH, FF))
    up = low_back(project(normed_ffw, up_weight, 5, 4 * MODEL_WIDTH + query_width, MODEL_WIDTH, query_width + 2 * key_span_width + MODEL_WIDTH + FF, FF))
    hidden = lower_factor(jax.nn.gelu(gate, approximate=True) * up)
    ffw_out = low_back(project(hidden, down_weight, 6, 5 * MODEL_WIDTH + query_width, FF, query_width + 2 * key_span_width + MODEL_WIDTH + 2 * FF, MODEL_WIDTH))
    return middle + normalize(ffw_out, fourth_gain)

def reference(inputs, cotangent, pre_attention, post_attention, pre_feedforward, post_feedforward, query_weight, key_matrix, value_matrix, output_weight, gate_weight, up_weight, down_weight, adapter_down, adapter_up, prefix_lengths, adapter_choice):
    weights = tuple((w.astype(jnp.float32) for w in (query_weight, key_matrix, value_matrix, output_weight, gate_weight, up_weight, down_weight)))
    gains = tuple((g.astype(jnp.float32) for g in (pre_attention, post_attention, pre_feedforward, post_feedforward)))
    down_table = adapter_down.astype(jnp.float32)
    up_table = adapter_up.astype(jnp.float32)
    count = MB * SEQS
    sources = inputs.astype(jnp.float32).reshape(count, SEQUENCE_LENGTH, MODEL_WIDTH)
    upstream = cotangent.astype(jnp.float32).reshape(count, SEQUENCE_LENGTH, MODEL_WIDTH)
    prefixes = prefix_lengths.reshape(count).astype(jnp.int32)
    pick_rows = adapter_choice.reshape(count, 7).astype(jnp.int32)

    def step(carry, item):
        source, seed_grad, prefix_length, picks = item

        def run(source_in, down_in, up_in):
            return layer(source_in, down_in, up_in, weights, gains, prefix_length, picks)
        result, pull = jax.vjp(run, source, down_table, up_table)
        grad_source, grad_down, grad_up = pull(seed_grad)
        return ((carry[0] + grad_down, carry[1] + grad_up), (result.astype(jnp.bfloat16), grad_source.astype(jnp.bfloat16)))
    start_index = (jnp.zeros(down_table.shape, jnp.float32), jnp.zeros(up_table.shape, jnp.float32))
    totals, produced = lax.scan(step, start_index, (sources, upstream, prefixes, pick_rows))
    outputs = produced[0].reshape(MB, SEQS, SEQUENCE_LENGTH, MODEL_WIDTH)
    input_gradient = produced[1].reshape(MB, SEQS, SEQUENCE_LENGTH, MODEL_WIDTH)
    return (outputs, input_gradient, totals[0], totals[1])
```

```python
import jax
import jax.numpy as jnp
from jax import lax
from jax.sharding import PartitionSpec as P

MODEL_WIDTH = 2304
QUERY_HEADS_COUNT = 8
KEY_VALUE_HEADS = 4
HEAD_SIZE = 256
FF = 9216


HIGH = lax.Precision.HIGHEST
EPSILON = 1e-06
SOFT_CAP = 50.0
WIDE = jnp.float32
NARROW = jnp.bfloat16


def normalize(value, gain):
    factor = lax.rsqrt(jnp.mean(value * value, axis=-1, keepdims=True) + EPSILON)
    return value * factor * gain


def normalize_back(value, gain, upstream):
    factor = lax.rsqrt(jnp.mean(value * value, axis=-1, keepdims=True) + EPSILON)
    scaled = upstream * gain
    inner = jnp.mean(value * scaled, axis=-1, keepdims=True)
    return factor * scaled - value * (factor * factor * factor) * inner


def angles(positions):
    half = HEAD_SIZE // 2
    rates = 10000.0 ** (-(jnp.arange(half, dtype=WIDE) * 2.0) / HEAD_SIZE)
    turns = positions.astype(WIDE)[:, None] * rates[None, :]
    return (jnp.cos(turns)[:, None, :], jnp.sin(turns)[:, None, :])


def apply_rotation(head_stack, cosine_table, sine_table):
    half = HEAD_SIZE // 2
    first = head_stack[..., :half]
    second = head_stack[..., half:]
    return jnp.concatenate(
        [first * cosine_table - second * sine_table, second * cosine_table + first * sine_table],
        axis=-1,
    )


def rotate_back(grads, cosine_table, sine_table):
    half = HEAD_SIZE // 2
    first = grads[..., :half]
    second = grads[..., half:]
    return jnp.concatenate(
        [first * cosine_table + second * sine_table, second * cosine_table - first * sine_table],
        axis=-1,
    )


def pick(table, index, start_index, size):
    return lax.dynamic_slice(table, (index, 0, start_index), (1, table.shape[1], size))[0]


def deposit(total, start_index, piece):
    return lax.dynamic_update_slice(total, piece, (0, start_index))


def segment_of(columns, widths):
    bounds = []
    edge = 0
    for width in widths[:-1]:
        edge += width
        bounds.append(edge)
    seg = jnp.zeros(columns.shape, jnp.int32)
    for edge in bounds:
        seg = seg + (columns >= edge).astype(jnp.int32)
    return seg


def spread(compact, choices, widths, adapters):
    flat = lax.axis_index(("dp", "seq", "mp"))
    cols = compact.shape[-1]
    columns = flat * cols + jnp.arange(cols, dtype=jnp.int32)
    seg = segment_of(columns, widths)
    chosen = jnp.take_along_axis(
        choices[:, :, None, :], jnp.broadcast_to(seg[None, None, :, None], choices.shape[:2] + (cols, 1)), axis=3
    )[..., 0]
    hits = chosen[None] == jnp.arange(adapters, dtype=jnp.int32)[:, None, None, None]
    picked = jnp.where(hits[:, :, None], compact[None], 0.0)
    return jnp.sum(picked, axis=(1, 3))


def settle(compact, choices, widths, adapters):
    mbs, rows, cols = compact.shape
    groups = lax.axis_size("dp")
    inner = lax.axis_size("seq") * lax.axis_size("mp")
    chunk = cols // (groups * inner)
    arranged = compact.reshape(mbs, rows, groups, inner, chunk)
    reduced = lax.psum_scatter(arranged, ("seq", "mp"), scatter_dimension=3, tiled=True)
    reduced = reduced.reshape(mbs, rows, groups, chunk)
    swapped = lax.all_to_all(reduced, "dp", 2, 2, tiled=True)
    return spread(swapped, choices, widths, adapters)


def activate(gate_value, up_value):
    return jax.nn.gelu(gate_value, approximate=True) * up_value


def combine_rows(main_part, inner_part):
    return lax.psum((main_part, inner_part), "mp")


def combine_input(partial_value):
    return lax.psum(partial_value, "mp")


def column_forward(inputs_low, weight, down_part, up_part):
    main = jnp.dot(inputs_low, weight, preferred_element_type=WIDE)
    inner = jnp.einsum("td,rd->tr", inputs_low, down_part, preferred_element_type=WIDE).astype(
        NARROW
    )
    return (main + jnp.dot(inner, up_part, preferred_element_type=WIDE), inner)


def row_forward(inputs_low, weight, down_part, up_part):
    main_part = jnp.dot(inputs_low, weight, preferred_element_type=WIDE)
    inner_part = jnp.einsum("tq,rq->tr", inputs_low, down_part, preferred_element_type=WIDE)
    main, inner = combine_rows(main_part, inner_part)
    inner_low = inner.astype(NARROW)
    return (main + jnp.dot(inner_low, up_part, preferred_element_type=WIDE), inner_low)


def column_back(grad_out, weight, down_part, up_part, inputs_low, inner_low):
    inner_grad = jnp.einsum("to,ro->tr", grad_out, up_part, preferred_element_type=WIDE)
    back = jnp.einsum("to,do->td", grad_out, weight, preferred_element_type=WIDE)
    back = back + jnp.dot(inner_grad, down_part.astype(WIDE), precision=HIGH)
    down_grad = jnp.einsum("tr,td->rd", inner_grad, inputs_low.astype(WIDE), precision=HIGH)
    up_grad = jnp.einsum("tr,to->ro", inner_low, grad_out, preferred_element_type=WIDE)
    return (back, down_grad, up_grad)


def row_back(grad_out, weight, down_part, up_part, inputs_low, inner_low, part, half):
    inner_grad = jnp.einsum("td,rd->tr", grad_out, up_part, preferred_element_type=WIDE)
    back = jnp.einsum("td,qd->tq", grad_out, weight, preferred_element_type=WIDE)
    back = back + jnp.dot(inner_grad, down_part.astype(WIDE), precision=HIGH)
    down_grad = jnp.einsum("tr,tq->rq", inner_grad, inputs_low.astype(WIDE), precision=HIGH)
    own_columns = lax.dynamic_slice_in_dim(grad_out, part * half, half, 1)
    up_grad = jnp.einsum("tr,tc->rc", inner_low, own_columns, preferred_element_type=WIDE)
    return (back, down_grad, up_grad)


def shards(
    inputs,
    cotangent,
    pre_attention,
    post_attention,
    pre_feedforward,
    post_feedforward,
    query_weight,
    key_matrix,
    value_matrix,
    output_weight,
    gate_weight,
    up_weight,
    down_weight,
    adapter_down,
    adapter_up,
    prefix_lengths,
    adapter_choice,
):
    parts = lax.axis_size("mp")
    part = lax.axis_index("mp")
    rows = inputs.shape[2]
    length = rows * lax.axis_size("seq")
    positions = lax.axis_index("seq") * rows + jnp.arange(rows, dtype=jnp.int32)
    key_positions = jnp.arange(length, dtype=jnp.int32)
    cosine_table, sine_table = angles(positions)
    query_width = QUERY_HEADS_COUNT * HEAD_SIZE
    key_span_width = KEY_VALUE_HEADS * HEAD_SIZE
    query_local = query_width // parts
    key_local = key_span_width // parts
    hidden_local = FF // parts
    half = MODEL_WIDTH // parts
    head_groups = QUERY_HEADS_COUNT // KEY_VALUE_HEADS
    query_heads = query_local // HEAD_SIZE
    key_heads = key_local // HEAD_SIZE
    scale = HEAD_SIZE ** (-0.5)
    in_output = 3 * MODEL_WIDTH + part * query_local
    in_gate = 3 * MODEL_WIDTH + query_width
    in_up = 4 * MODEL_WIDTH + query_width
    in_down = 5 * MODEL_WIDTH + query_width + part * hidden_local
    out_query = part * query_local
    out_key = query_width + part * key_local
    out_value = query_width + key_span_width + part * key_local
    out_output = query_width + 2 * key_span_width
    out_gate = query_width + 2 * key_span_width + MODEL_WIDTH + part * hidden_local
    out_up = query_width + 2 * key_span_width + MODEL_WIDTH + FF + part * hidden_local
    out_down = query_width + 2 * key_span_width + MODEL_WIDTH + 2 * FF
    down_list = []
    up_list = []
    results = []
    input_grads = []
    for batch in range(inputs.shape[0]):
        first = (
            lax.all_gather(query_weight, ("dp", "seq"), axis=0, tiled=True),
            lax.all_gather(key_matrix, ("dp", "seq"), axis=0, tiled=True),
            lax.all_gather(value_matrix, ("dp", "seq"), axis=0, tiled=True),
            lax.all_gather(output_weight, ("dp", "seq"), axis=1, tiled=True),
            lax.all_gather(gate_weight, ("dp", "seq"), axis=0, tiled=True),
            lax.all_gather(up_weight, ("dp", "seq"), axis=0, tiled=True),
            lax.all_gather(down_weight, ("dp", "seq"), axis=1, tiled=True),
        )
        query_full, key_full, value_full, output_full, gate_full, up_full, down_full = first
        slots = adapter_choice[batch, 0]
        prefix_length = prefix_lengths[batch, 0]
        down_query = pick(adapter_down, slots[0], 0, MODEL_WIDTH)
        down_key = pick(adapter_down, slots[1], MODEL_WIDTH, MODEL_WIDTH)
        down_value = pick(adapter_down, slots[2], 2 * MODEL_WIDTH, MODEL_WIDTH)
        down_output = pick(adapter_down, slots[3], in_output, query_local)
        down_gate = pick(adapter_down, slots[4], in_gate, MODEL_WIDTH)
        down_up = pick(adapter_down, slots[5], in_up, MODEL_WIDTH)
        down_down = pick(adapter_down, slots[6], in_down, hidden_local)
        up_query = pick(adapter_up, slots[0], out_query, query_local)
        up_key = pick(adapter_up, slots[1], out_key, key_local)
        up_value = pick(adapter_up, slots[2], out_value, key_local)
        up_output = pick(adapter_up, slots[3], out_output, MODEL_WIDTH)
        up_gate = pick(adapter_up, slots[4], out_gate, hidden_local)
        up_upper = pick(adapter_up, slots[5], out_up, hidden_local)
        up_down = pick(adapter_up, slots[6], out_down, MODEL_WIDTH)
        source = inputs[batch, 0].astype(WIDE)
        normed = normalize(source, pre_attention).astype(NARROW)
        query, inner_query = column_forward(normed, query_full, down_query, up_query)
        key_rows, inner_key = column_forward(normed, key_full, down_key, up_key)
        value_rows, inner_value = column_forward(normed, value_full, down_value, up_value)
        rotated_query = apply_rotation(
            query.reshape(rows, query_heads, HEAD_SIZE), cosine_table, sine_table
        ).astype(NARROW)
        rotated_keys = (
            apply_rotation(key_rows.reshape(rows, key_heads, HEAD_SIZE), cosine_table, sine_table)
            .astype(NARROW)
            .reshape(rows, key_local)
        )
        values_low = value_rows.astype(NARROW)
        both_all = lax.all_gather(jnp.stack([rotated_keys, values_low]), "seq", axis=1, tiled=True)
        keys_all, values_all = both_all[0], both_all[1]
        query_four = rotated_query.reshape(rows, key_heads, head_groups, HEAD_SIZE)
        keys_three = keys_all.reshape(length, key_heads, HEAD_SIZE)
        values_three = values_all.reshape(length, key_heads, HEAD_SIZE)
        visible = (key_positions[None, :] <= positions[:, None]) | (
            key_positions[None, :] < prefix_length
        )
        raw = (
            jnp.einsum("tkgd,skd->kgts", query_four, keys_three, preferred_element_type=WIDE)
            * scale
        )
        masked = jnp.where(visible, SOFT_CAP * jnp.tanh(raw / SOFT_CAP), -1e30)
        top = jnp.max(masked, axis=-1, keepdims=True)
        expo = jnp.exp(masked - top)
        total = jnp.sum(expo, axis=-1, keepdims=True)
        log_total = top + jnp.log(total)
        prob_low = (expo / total).astype(NARROW)
        head_stack = jnp.einsum(
            "kgts,skd->tkgd", prob_low, values_three, preferred_element_type=WIDE
        )
        head_stack = head_stack.reshape(rows, query_local).astype(NARROW)
        attention_out, inner_output = row_forward(head_stack, output_full, down_output, up_output)
        middle = source + normalize(attention_out, post_attention)
        normed_ffw = normalize(middle, pre_feedforward).astype(NARROW)
        gate, inner_gate = column_forward(normed_ffw, gate_full, down_gate, up_gate)
        upper, inner_upper = column_forward(normed_ffw, up_full, down_up, up_upper)
        hidden = activate(gate, upper).astype(NARROW)
        ffw_out, inner_down = row_forward(hidden, down_full, down_down, up_down)
        results.append((middle + normalize(ffw_out, post_feedforward)).astype(NARROW))
        second = (
            lax.all_gather(query_weight, ("dp", "seq"), axis=0, tiled=True),
            lax.all_gather(key_matrix, ("dp", "seq"), axis=0, tiled=True),
            lax.all_gather(value_matrix, ("dp", "seq"), axis=0, tiled=True),
            lax.all_gather(output_weight, ("dp", "seq"), axis=1, tiled=True),
            lax.all_gather(gate_weight, ("dp", "seq"), axis=0, tiled=True),
            lax.all_gather(up_weight, ("dp", "seq"), axis=0, tiled=True),
            lax.all_gather(down_weight, ("dp", "seq"), axis=1, tiled=True),
        )
        query_back, key_back, value_back, output_back, gate_back, up_back, down_back = second
        grad_down = jnp.zeros(adapter_down.shape[1:], WIDE)
        grad_up = jnp.zeros(adapter_up.shape[1:], WIDE)
        seed_grad = cotangent[batch, 0].astype(WIDE)
        grad_ffw = normalize_back(ffw_out, post_feedforward, seed_grad).astype(NARROW)
        grad_hidden, piece_down, piece_up = row_back(
            grad_ffw, down_back, down_down, up_down, hidden, inner_down, part, half
        )
        grad_down = deposit(grad_down, in_down, piece_down)
        grad_up = deposit(grad_up, out_down + part * half, piece_up)
        pull = jax.vjp(activate, gate, upper)[1]
        grad_gate, grad_upper = pull(grad_hidden)
        grad_gate = grad_gate.astype(NARROW)
        grad_upper = grad_upper.astype(NARROW)
        back_gate, piece_down, piece_up = column_back(
            grad_gate, gate_back, down_gate, up_gate, normed_ffw, inner_gate
        )
        grad_down = deposit(grad_down, in_gate, piece_down)
        grad_up = deposit(grad_up, out_gate, piece_up)
        back_upper, piece_down, piece_up = column_back(
            grad_upper, up_back, down_up, up_upper, normed_ffw, inner_upper
        )
        grad_down = deposit(grad_down, in_up, piece_down)
        grad_up = deposit(grad_up, out_up, piece_up)
        grad_normed_ffw = combine_input(back_gate + back_upper)
        grad_middle = seed_grad + normalize_back(middle, pre_feedforward, grad_normed_ffw)
        grad_attention = normalize_back(attention_out, post_attention, grad_middle).astype(NARROW)
        grad_heads, piece_down, piece_up = row_back(
            grad_attention,
            output_back,
            down_output,
            up_output,
            head_stack,
            inner_output,
            part,
            half,
        )
        grad_down = deposit(grad_down, in_output, piece_down)
        grad_up = deposit(grad_up, out_output + part * half, piece_up)
        grad_heads_four = grad_heads.astype(NARROW).reshape(rows, key_heads, head_groups, HEAD_SIZE)
        prob = jnp.exp(masked - log_total)
        grad_prob = jnp.einsum(
            "tkgd,skd->kgts", grad_heads_four, values_three, preferred_element_type=WIDE
        )
        grad_capped = prob * (grad_prob - jnp.sum(prob * grad_prob, axis=-1, keepdims=True))
        bend = jnp.tanh(raw / SOFT_CAP)
        grad_raw = (grad_capped * (1.0 - bend * bend)).astype(NARROW)
        grad_query_rot = (
            jnp.einsum("kgts,skd->tkgd", grad_raw, keys_three, preferred_element_type=WIDE) * scale
        )
        grad_key_part = (
            jnp.einsum("kgts,tkgd->skd", grad_raw, query_four, preferred_element_type=WIDE) * scale
        )
        grad_value_part = jnp.einsum(
            "kgts,tkgd->skd", prob_low, grad_heads_four, preferred_element_type=WIDE
        )
        both_grad = lax.psum_scatter(
            jnp.stack([grad_key_part.reshape(length, key_local), grad_value_part.reshape(length, key_local)]),
            "seq",
            scatter_dimension=1,
            tiled=True,
        )
        key_grad, value_grad = both_grad[0], both_grad[1]
        grad_query = (
            rotate_back(
                grad_query_rot.reshape(rows, query_heads, HEAD_SIZE), cosine_table, sine_table
            )
            .reshape(rows, query_local)
            .astype(NARROW)
        )
        grad_key = (
            rotate_back(key_grad.reshape(rows, key_heads, HEAD_SIZE), cosine_table, sine_table)
            .reshape(rows, key_local)
            .astype(NARROW)
        )
        grad_value = value_grad.astype(NARROW)
        back_query, piece_down, piece_up = column_back(
            grad_query, query_back, down_query, up_query, normed, inner_query
        )
        grad_down = deposit(grad_down, 0, piece_down)
        grad_up = deposit(grad_up, out_query, piece_up)
        back_key, piece_down, piece_up = column_back(
            grad_key, key_back, down_key, up_key, normed, inner_key
        )
        grad_down = deposit(grad_down, MODEL_WIDTH, piece_down)
        grad_up = deposit(grad_up, out_key, piece_up)
        back_value, piece_down, piece_up = column_back(
            grad_value, value_back, down_value, up_value, normed, inner_value
        )
        grad_down = deposit(grad_down, 2 * MODEL_WIDTH, piece_down)
        grad_up = deposit(grad_up, out_value, piece_up)
        grad_normed = combine_input(back_query + back_key + back_value)
        down_list.append(grad_down)
        up_list.append(grad_up)
        input_grads.append(
            (grad_middle + normalize_back(source, pre_attention, grad_normed)).astype(NARROW)
        )
    choices = lax.all_gather(adapter_choice[:, 0], "dp", axis=1, tiled=False)
    down_widths = (MODEL_WIDTH, MODEL_WIDTH, MODEL_WIDTH, query_width, MODEL_WIDTH, MODEL_WIDTH, FF)
    up_widths = (query_width, key_span_width, key_span_width, MODEL_WIDTH, FF, FF, MODEL_WIDTH)
    down_total = settle(jnp.stack(down_list), choices, down_widths, adapter_down.shape[0])
    up_total = settle(jnp.stack(up_list), choices, up_widths, adapter_up.shape[0])
    outputs = jnp.stack(results)[:, None]
    input_gradient = jnp.stack(input_grads)[:, None]
    return (outputs, input_gradient, down_total, up_total)


def solution(mesh):
    return jax.shard_map(
        shards,
        mesh=mesh,
        in_specs=(
            P(None, "dp", "seq", None),
            P(None, "dp", "seq", None),
            P(),
            P(),
            P(),
            P(),
            P(("dp", "seq"), "mp"),
            P(("dp", "seq"), "mp"),
            P(("dp", "seq"), "mp"),
            P("mp", ("dp", "seq")),
            P(("dp", "seq"), "mp"),
            P(("dp", "seq"), "mp"),
            P("mp", ("dp", "seq")),
            P(),
            P(),
            P(None, "dp"),
            P(None, "dp", None),
        ),
        out_specs=(
            P(None, "dp", "seq", None),
            P(None, "dp", "seq", None),
            P(None, None, ("dp", "seq", "mp")),
            P(None, None, ("dp", "seq", "mp")),
        ),
        check_vma=False,
    )
```

```python
import jax
import jax.numpy as jnp
from jax import lax
from jax.sharding import PartitionSpec as P

MODEL_WIDTH = 2304
QUERY_HEADS_COUNT = 8
KEY_VALUE_HEADS = 4
HEAD_SIZE = 256
FF = 9216


HIGH = lax.Precision.HIGHEST
EPSILON = 1e-06
SOFT_CAP = 50.0
WIDE = jnp.float32
NARROW = jnp.bfloat16


def normalize(value, gain):
    factor = lax.rsqrt(jnp.mean(value * value, axis=-1, keepdims=True) + EPSILON)
    return value * factor * gain


def normalize_back(value, gain, upstream):
    factor = lax.rsqrt(jnp.mean(value * value, axis=-1, keepdims=True) + EPSILON)
    scaled = upstream * gain
    inner = jnp.mean(value * scaled, axis=-1, keepdims=True)
    return factor * scaled - value * (factor * factor * factor) * inner


def angles(positions):
    half = HEAD_SIZE // 2
    rates = 10000.0 ** (-(jnp.arange(half, dtype=WIDE) * 2.0) / HEAD_SIZE)
    turns = positions.astype(WIDE)[:, None] * rates[None, :]
    return (jnp.cos(turns)[:, None, :], jnp.sin(turns)[:, None, :])


def apply_rotation(head_stack, cosine_table, sine_table):
    half = HEAD_SIZE // 2
    first = head_stack[..., :half]
    second = head_stack[..., half:]
    return jnp.concatenate(
        [first * cosine_table - second * sine_table, second * cosine_table + first * sine_table],
        axis=-1,
    )


def rotate_back(grads, cosine_table, sine_table):
    half = HEAD_SIZE // 2
    first = grads[..., :half]
    second = grads[..., half:]
    return jnp.concatenate(
        [first * cosine_table + second * sine_table, second * cosine_table - first * sine_table],
        axis=-1,
    )


def pick(table, index, start_index, size):
    return lax.dynamic_slice(table, (index, 0, start_index), (1, table.shape[1], size))[0]


def picks(table, slots, start_index, size):
    return jnp.stack([pick(table, slots[e], start_index, size) for e in range(slots.shape[0])])


def place(total, piece, start_index):
    return lax.dynamic_update_slice(total, piece, (0, 0, start_index))


def place_own(total, piece, own, start_index):
    return lax.dynamic_update_slice(total, piece[None], (own, 0, start_index))


def activate(gate_value, up_value):
    return jax.nn.gelu(gate_value, approximate=True) * up_value


def segment_of(columns, widths):
    seg = jnp.zeros(columns.shape, jnp.int32)
    edge = 0
    for width in widths[:-1]:
        edge += width
        seg = seg + (columns >= edge).astype(jnp.int32)
    return seg


def settle(compact, choices, widths, adapters):
    mbs, seqs, rows, cols = compact.shape
    devices = lax.axis_size(("dp", "seq", "mp"))
    chunk = cols // devices
    arranged = compact.reshape(mbs, seqs, rows, devices, chunk)
    reduced = lax.psum_scatter(arranged, ("dp", "seq", "mp"), scatter_dimension=3, tiled=True)
    reduced = reduced.reshape(mbs, seqs, rows, chunk)
    flat = lax.axis_index(("dp", "seq", "mp"))
    columns = flat * chunk + jnp.arange(chunk, dtype=jnp.int32)
    seg = segment_of(columns, widths)
    chosen = jnp.take_along_axis(
        choices[:, :, None, :], jnp.broadcast_to(seg[None, None, :, None], (mbs, seqs, chunk, 1)), axis=3
    )[..., 0]
    hits = chosen[None] == jnp.arange(adapters, dtype=jnp.int32)[:, None, None, None]
    picked = jnp.where(hits[:, :, :, None, :], reduced[None], 0.0)
    return jnp.sum(picked, axis=(1, 2))


def to_owner(partial):
    mine = lax.psum_scatter(partial, "dp", scatter_dimension=0, tiled=True)[0]
    return lax.psum(mine, "mp")


def shards(
    inputs,
    cotangent,
    pre_attention,
    post_attention,
    pre_feedforward,
    post_feedforward,
    query_weight,
    key_matrix,
    value_matrix,
    output_weight,
    gate_weight,
    up_weight,
    down_weight,
    adapter_down,
    adapter_up,
    prefix_lengths,
    adapter_choice,
):
    groups = lax.axis_size("dp")
    parts = lax.axis_size("mp")
    blocks = lax.axis_size("seq")
    quarters = groups * parts
    own = lax.axis_index("dp")
    part = lax.axis_index("mp")
    quarter = part * groups + own
    rows = inputs.shape[2]
    length = rows * blocks
    positions = lax.axis_index("seq") * rows + jnp.arange(rows, dtype=jnp.int32)
    key_positions = jnp.arange(length, dtype=jnp.int32)
    cosine_table, sine_table = angles(positions)
    query_width = QUERY_HEADS_COUNT * HEAD_SIZE
    key_span_width = KEY_VALUE_HEADS * HEAD_SIZE
    query_local = query_width // quarters
    key_local = key_span_width // quarters
    hidden_local = FF // quarters
    half = MODEL_WIDTH // parts
    head_groups = QUERY_HEADS_COUNT // KEY_VALUE_HEADS
    query_heads = query_local // HEAD_SIZE
    key_heads = key_local // HEAD_SIZE
    row_block = MODEL_WIDTH // (groups * blocks)
    scale = HEAD_SIZE ** (-0.5)
    in_output = 3 * MODEL_WIDTH + quarter * query_local
    in_gate = 3 * MODEL_WIDTH + query_width
    in_up = 4 * MODEL_WIDTH + query_width
    in_down = 5 * MODEL_WIDTH + query_width + quarter * hidden_local
    out_query = quarter * query_local
    out_key = query_width + quarter * key_local
    out_value = query_width + key_span_width + quarter * key_local
    out_output = query_width + 2 * key_span_width
    out_gate = query_width + 2 * key_span_width + MODEL_WIDTH + quarter * hidden_local
    out_up = query_width + 2 * key_span_width + MODEL_WIDTH + FF + quarter * hidden_local
    out_down = query_width + 2 * key_span_width + MODEL_WIDTH + 2 * FF
    tokens = groups * rows

    def permute(value):
        lead = value.shape[:-1]
        moved = value.reshape(lead + (groups, blocks, row_block))
        return jnp.swapaxes(moved, -3, -2).reshape(lead + (MODEL_WIDTH,))

    def unpermute(value):
        lead = value.shape[:-1]
        moved = value.reshape(lead + (blocks, groups, row_block))
        return jnp.swapaxes(moved, -3, -2).reshape(lead + (MODEL_WIDTH,))

    def column_weight(weight):
        swapped = lax.all_to_all(weight, "dp", 1, 0, tiled=True)
        return lax.all_gather(swapped, "seq", axis=0, tiled=True)

    def row_weight(weight):
        swapped = lax.all_to_all(weight, "dp", 0, 1, tiled=True)
        return lax.all_gather(swapped, "seq", axis=1, tiled=True)

    query_full = column_weight(query_weight)
    key_full = column_weight(key_matrix)
    value_full = column_weight(value_matrix)
    output_full = row_weight(output_weight)
    gate_full = column_weight(gate_weight)
    up_full = column_weight(up_weight)
    down_full = row_weight(down_weight)

    sources_all = lax.all_gather(inputs[:, 0], "dp", axis=1, tiled=False)
    prefix_all = lax.all_gather(prefix_lengths[:, 0], "dp", axis=1, tiled=False)
    choices = lax.all_gather(adapter_choice[:, 0], "dp", axis=1, tiled=False)

    def column_forward(inputs_low, weight, down_part, up_part):
        main = jnp.dot(permute(inputs_low).reshape(tokens, MODEL_WIDTH), weight, preferred_element_type=WIDE)
        inner = jnp.einsum("etd,erd->etr", inputs_low, down_part, preferred_element_type=WIDE).astype(NARROW)
        low = jnp.einsum("etr,ero->eto", inner, up_part, preferred_element_type=WIDE)
        return (main.reshape(groups, rows, -1) + low, inner)

    def row_forward(inputs_low, weight, down_part, up_own):
        width = inputs_low.shape[-1]
        main_part = jnp.dot(inputs_low.reshape(tokens, width), weight, preferred_element_type=WIDE)
        inner_part = jnp.einsum("etq,erq->etr", inputs_low, down_part, preferred_element_type=WIDE)
        both = jnp.concatenate([main_part.reshape(groups, rows, MODEL_WIDTH), inner_part], axis=-1)
        both = to_owner(both)
        main = unpermute(both[:, :MODEL_WIDTH])
        inner_low = both[:, MODEL_WIDTH:].astype(NARROW)
        return (main + jnp.dot(inner_low, up_own, preferred_element_type=WIDE), inner_low)

    def column_back(grad_out, weight, down_part, up_part, inputs_low, inner_low):
        inner_grad = jnp.einsum("eto,ero->etr", grad_out, up_part, preferred_element_type=WIDE)
        width = grad_out.shape[-1]
        back = jnp.einsum("to,do->td", grad_out.reshape(tokens, width), weight, preferred_element_type=WIDE)
        back = unpermute(back.reshape(groups, rows, MODEL_WIDTH))
        back = back + jnp.einsum("etr,erd->etd", inner_grad, down_part.astype(WIDE), precision=HIGH)
        down_grad = jnp.einsum("etr,etd->erd", inner_grad, inputs_low.astype(WIDE), precision=HIGH)
        up_grad = jnp.einsum("etr,eto->ero", inner_low, grad_out, preferred_element_type=WIDE)
        return (back, down_grad, up_grad)

    def row_back(grad_all, grad_own, weight, down_part, up_part, inputs_low, inner_own):
        inner_grad = jnp.einsum("etd,erd->etr", grad_all, up_part, preferred_element_type=WIDE)
        back = jnp.einsum(
            "td,qd->tq", permute(grad_all).reshape(tokens, MODEL_WIDTH), weight, preferred_element_type=WIDE
        )
        back = back.reshape(groups, rows, -1)
        back = back + jnp.einsum("etr,erq->etq", inner_grad, down_part.astype(WIDE), precision=HIGH)
        down_grad = jnp.einsum("etr,etq->erq", inner_grad, inputs_low.astype(WIDE), precision=HIGH)
        own_columns = lax.dynamic_slice_in_dim(grad_own, part * half, half, 1)
        up_grad = jnp.einsum("tr,tc->rc", inner_own, own_columns, preferred_element_type=WIDE)
        return (back, down_grad, up_grad)

    down_list = []
    up_list = []
    results = []
    input_grads = []
    for batch in range(inputs.shape[0]):
        slots = choices[batch]
        own_slots = adapter_choice[batch, 0]
        prefix_length = prefix_all[batch]
        down_query = picks(adapter_down, slots[:, 0], 0, MODEL_WIDTH)
        down_key = picks(adapter_down, slots[:, 1], MODEL_WIDTH, MODEL_WIDTH)
        down_value = picks(adapter_down, slots[:, 2], 2 * MODEL_WIDTH, MODEL_WIDTH)
        down_output = picks(adapter_down, slots[:, 3], in_output, query_local)
        down_gate = picks(adapter_down, slots[:, 4], in_gate, MODEL_WIDTH)
        down_up = picks(adapter_down, slots[:, 5], in_up, MODEL_WIDTH)
        down_down = picks(adapter_down, slots[:, 6], in_down, hidden_local)
        up_query = picks(adapter_up, slots[:, 0], out_query, query_local)
        up_key = picks(adapter_up, slots[:, 1], out_key, key_local)
        up_value = picks(adapter_up, slots[:, 2], out_value, key_local)
        up_output = picks(adapter_up, slots[:, 3], out_output, MODEL_WIDTH)
        up_gate = picks(adapter_up, slots[:, 4], out_gate, hidden_local)
        up_upper = picks(adapter_up, slots[:, 5], out_up, hidden_local)
        up_down = picks(adapter_up, slots[:, 6], out_down, MODEL_WIDTH)
        up_output_own = pick(adapter_up, own_slots[3], out_output, MODEL_WIDTH)
        up_down_own = pick(adapter_up, own_slots[6], out_down, MODEL_WIDTH)

        source = inputs[batch, 0].astype(WIDE)
        normed = normalize(sources_all[batch].astype(WIDE), pre_attention).astype(NARROW)
        query, inner_query = column_forward(normed, query_full, down_query, up_query)
        key_rows, inner_key = column_forward(normed, key_full, down_key, up_key)
        value_rows, inner_value = column_forward(normed, value_full, down_value, up_value)
        rotated_query = apply_rotation(
            query.reshape(groups, rows, query_heads, HEAD_SIZE), cosine_table, sine_table
        ).astype(NARROW)
        rotated_keys = (
            apply_rotation(key_rows.reshape(groups, rows, key_heads, HEAD_SIZE), cosine_table, sine_table)
            .astype(NARROW)
            .reshape(groups, rows, key_local)
        )
        values_low = value_rows.astype(NARROW)
        both_all = lax.all_gather(jnp.stack([rotated_keys, values_low]), "seq", axis=2, tiled=True)
        keys_three = both_all[0].reshape(groups, length, key_heads, HEAD_SIZE)
        values_three = both_all[1].reshape(groups, length, key_heads, HEAD_SIZE)
        query_four = rotated_query.reshape(groups, rows, key_heads, head_groups, HEAD_SIZE)
        visible = (key_positions[None, None, :] <= positions[None, :, None]) | (
            key_positions[None, None, :] < prefix_length[:, None, None]
        )
        visible = visible[:, None, None]
        raw = (
            jnp.einsum("etkgd,eskd->ekgts", query_four, keys_three, preferred_element_type=WIDE)
            * scale
        )
        masked = jnp.where(visible, SOFT_CAP * jnp.tanh(raw / SOFT_CAP), -1e30)
        top = jnp.max(masked, axis=-1, keepdims=True)
        expo = jnp.exp(masked - top)
        total = jnp.sum(expo, axis=-1, keepdims=True)
        log_total = top + jnp.log(total)
        prob_low = (expo / total).astype(NARROW)
        head_stack = jnp.einsum(
            "ekgts,eskd->etkgd", prob_low, values_three, preferred_element_type=WIDE
        )
        head_stack = head_stack.reshape(groups, rows, query_local).astype(NARROW)
        attention_out, inner_output = row_forward(head_stack, output_full, down_output, up_output_own)
        middle = source + normalize(attention_out, post_attention)
        normed_ffw_own = normalize(middle, pre_feedforward).astype(NARROW)
        normed_ffw = lax.all_gather(normed_ffw_own, "dp", axis=0, tiled=False)
        gate, inner_gate = column_forward(normed_ffw, gate_full, down_gate, up_gate)
        upper, inner_upper = column_forward(normed_ffw, up_full, down_up, up_upper)
        hidden = activate(gate, upper).astype(NARROW)
        ffw_out, inner_down = row_forward(hidden, down_full, down_down, up_down_own)
        results.append((middle + normalize(ffw_out, post_feedforward)).astype(NARROW))

        grad_down = jnp.zeros((groups,) + adapter_down.shape[1:], WIDE)
        grad_up = jnp.zeros((groups,) + adapter_up.shape[1:], WIDE)
        seed_grad = cotangent[batch, 0].astype(WIDE)
        grad_ffw_own = normalize_back(ffw_out, post_feedforward, seed_grad).astype(NARROW)
        grad_ffw = lax.all_gather(grad_ffw_own, "dp", axis=0, tiled=False)
        grad_hidden, piece_down, piece_up = row_back(
            grad_ffw, grad_ffw_own, down_full, down_down, up_down, hidden, inner_down
        )
        grad_down = place(grad_down, piece_down, in_down)
        grad_up = place_own(grad_up, piece_up, own, out_down + part * half)
        pull = jax.vjp(activate, gate, upper)[1]
        grad_gate, grad_upper = pull(grad_hidden)
        grad_gate = grad_gate.astype(NARROW)
        grad_upper = grad_upper.astype(NARROW)
        back_gate, piece_down, piece_up = column_back(
            grad_gate, gate_full, down_gate, up_gate, normed_ffw, inner_gate
        )
        grad_down = place(grad_down, piece_down, in_gate)
        grad_up = place(grad_up, piece_up, out_gate)
        back_upper, piece_down, piece_up = column_back(
            grad_upper, up_full, down_up, up_upper, normed_ffw, inner_upper
        )
        grad_down = place(grad_down, piece_down, in_up)
        grad_up = place(grad_up, piece_up, out_up)
        grad_normed_ffw = to_owner(back_gate + back_upper)
        grad_middle = seed_grad + normalize_back(middle, pre_feedforward, grad_normed_ffw)
        grad_attention_own = normalize_back(attention_out, post_attention, grad_middle).astype(NARROW)
        grad_attention = lax.all_gather(grad_attention_own, "dp", axis=0, tiled=False)
        grad_heads, piece_down, piece_up = row_back(
            grad_attention,
            grad_attention_own,
            output_full,
            down_output,
            up_output,
            head_stack,
            inner_output,
        )
        grad_down = place(grad_down, piece_down, in_output)
        grad_up = place_own(grad_up, piece_up, own, out_output + part * half)
        grad_heads_four = grad_heads.astype(NARROW).reshape(groups, rows, key_heads, head_groups, HEAD_SIZE)
        prob = jnp.exp(masked - log_total)
        grad_prob = jnp.einsum(
            "etkgd,eskd->ekgts", grad_heads_four, values_three, preferred_element_type=WIDE
        )
        grad_capped = prob * (grad_prob - jnp.sum(prob * grad_prob, axis=-1, keepdims=True))
        bend = jnp.tanh(raw / SOFT_CAP)
        grad_raw = (grad_capped * (1.0 - bend * bend)).astype(NARROW)
        grad_query_rot = (
            jnp.einsum("ekgts,eskd->etkgd", grad_raw, keys_three, preferred_element_type=WIDE) * scale
        )
        grad_key_part = (
            jnp.einsum("ekgts,etkgd->eskd", grad_raw, query_four, preferred_element_type=WIDE) * scale
        )
        grad_value_part = jnp.einsum(
            "ekgts,etkgd->eskd", prob_low, grad_heads_four, preferred_element_type=WIDE
        )
        both_grad = lax.psum_scatter(
            jnp.stack(
                [
                    grad_key_part.reshape(groups, length, key_local),
                    grad_value_part.reshape(groups, length, key_local),
                ]
            ),
            "seq",
            scatter_dimension=2,
            tiled=True,
        )
        key_grad, value_grad = both_grad[0], both_grad[1]
        grad_query = (
            rotate_back(
                grad_query_rot.reshape(groups, rows, query_heads, HEAD_SIZE), cosine_table, sine_table
            )
            .reshape(groups, rows, query_local)
            .astype(NARROW)
        )
        grad_key = (
            rotate_back(key_grad.reshape(groups, rows, key_heads, HEAD_SIZE), cosine_table, sine_table)
            .reshape(groups, rows, key_local)
            .astype(NARROW)
        )
        grad_value = value_grad.astype(NARROW)
        back_query, piece_down, piece_up = column_back(
            grad_query, query_full, down_query, up_query, normed, inner_query
        )
        grad_down = place(grad_down, piece_down, 0)
        grad_up = place(grad_up, piece_up, out_query)
        back_key, piece_down, piece_up = column_back(
            grad_key, key_full, down_key, up_key, normed, inner_key
        )
        grad_down = place(grad_down, piece_down, MODEL_WIDTH)
        grad_up = place(grad_up, piece_up, out_key)
        back_value, piece_down, piece_up = column_back(
            grad_value, value_full, down_value, up_value, normed, inner_value
        )
        grad_down = place(grad_down, piece_down, 2 * MODEL_WIDTH)
        grad_up = place(grad_up, piece_up, out_value)
        grad_normed = to_owner(back_query + back_key + back_value)
        down_list.append(grad_down)
        up_list.append(grad_up)
        input_grads.append(
            (grad_middle + normalize_back(source, pre_attention, grad_normed)).astype(NARROW)
        )
    down_widths = (MODEL_WIDTH, MODEL_WIDTH, MODEL_WIDTH, query_width, MODEL_WIDTH, MODEL_WIDTH, FF)
    up_widths = (query_width, key_span_width, key_span_width, MODEL_WIDTH, FF, FF, MODEL_WIDTH)
    down_total = settle(jnp.stack(down_list), choices, down_widths, adapter_down.shape[0])
    up_total = settle(jnp.stack(up_list), choices, up_widths, adapter_up.shape[0])
    outputs = jnp.stack(results)[:, None]
    input_gradient = jnp.stack(input_grads)[:, None]
    return (outputs, input_gradient, down_total, up_total)


def solution(mesh):
    return jax.shard_map(
        shards,
        mesh=mesh,
        in_specs=(
            P(None, "dp", "seq", None),
            P(None, "dp", "seq", None),
            P(),
            P(),
            P(),
            P(),
            P(("dp", "seq"), "mp"),
            P(("dp", "seq"), "mp"),
            P(("dp", "seq"), "mp"),
            P("mp", ("dp", "seq")),
            P(("dp", "seq"), "mp"),
            P(("dp", "seq"), "mp"),
            P("mp", ("dp", "seq")),
            P(),
            P(),
            P(None, "dp"),
            P(None, "dp", None),
        ),
        out_specs=(
            P(None, "dp", "seq", None),
            P(None, "dp", "seq", None),
            P(None, None, ("dp", "seq", "mp")),
            P(None, None, ("dp", "seq", "mp")),
        ),
        check_vma=False,
    )
```

```python
import numpy as np
import jax
import jax.numpy as jnp
from jax import lax
from jax.sharding import PartitionSpec as P

MODEL_WIDTH = 2304
QUERY_HEADS_COUNT = 8
KEY_VALUE_HEADS = 4
HEAD_SIZE = 256
FF = 9216


HIGH = lax.Precision.HIGHEST
EPSILON = 1e-06
SOFT_CAP = 50.0
WIDE = jnp.float32
NARROW = jnp.bfloat16


def normalize(value, gain):
    factor = lax.rsqrt(jnp.mean(value * value, axis=-1, keepdims=True) + EPSILON)
    return value * factor * gain


def normalize_back(value, gain, upstream):
    factor = lax.rsqrt(jnp.mean(value * value, axis=-1, keepdims=True) + EPSILON)
    scaled = upstream * gain
    inner = jnp.mean(value * scaled, axis=-1, keepdims=True)
    return factor * scaled - value * (factor * factor * factor) * inner


def angles(positions):
    half = HEAD_SIZE // 2
    rates = 10000.0 ** (-(jnp.arange(half, dtype=WIDE) * 2.0) / HEAD_SIZE)
    turns = positions.astype(WIDE)[:, None] * rates[None, :]
    return (jnp.cos(turns)[:, None, :], jnp.sin(turns)[:, None, :])


def apply_rotation(head_stack, cosine_table, sine_table):
    half = HEAD_SIZE // 2
    first = head_stack[..., :half]
    second = head_stack[..., half:]
    return jnp.concatenate(
        [first * cosine_table - second * sine_table, second * cosine_table + first * sine_table],
        axis=-1,
    )


def rotate_back(grads, cosine_table, sine_table):
    half = HEAD_SIZE // 2
    first = grads[..., :half]
    second = grads[..., half:]
    return jnp.concatenate(
        [first * cosine_table + second * sine_table, second * cosine_table - first * sine_table],
        axis=-1,
    )


def pick(table, index, start_index, size):
    return lax.dynamic_slice(table, (index, 0, start_index), (1, table.shape[1], size))[0]


def picks(table, slots, start_index, size):
    return jnp.stack([pick(table, slots[e], start_index, size) for e in range(slots.shape[0])])


def place(total, piece, start_index):
    return lax.dynamic_update_slice(total, piece, (0, 0, start_index))


def place_own(total, piece, own, start_index):
    return lax.dynamic_update_slice(total, piece[None], (own, 0, start_index))


def activate(gate_value, up_value):
    return jax.nn.gelu(gate_value, approximate=True) * up_value


def segment_of(columns, widths):
    seg = jnp.zeros(columns.shape, jnp.int32)
    edge = 0
    for width in widths[:-1]:
        edge += width
        seg = seg + (columns >= edge).astype(jnp.int32)
    return seg


def spread(compact, choices, widths, adapters, start):
    columns = start + jnp.arange(compact.shape[-1], dtype=jnp.int32)
    seg = segment_of(columns, widths)
    chosen = jnp.zeros((choices.shape[0], compact.shape[-1]), jnp.int32)
    for index in range(len(widths)):
        chosen = chosen + jnp.where(seg == index, choices[:, index : index + 1], 0)
    hits = chosen[None] == jnp.arange(adapters, dtype=jnp.int32)[:, None, None]
    picked = jnp.where(hits[:, :, None, :], compact[None], 0.0)
    return jnp.sum(picked, axis=1)


def snake(sizes):
    if not sizes:
        return [()]
    inner = snake(sizes[1:])
    order = []
    for value in range(sizes[0]):
        steps = inner if value % 2 == 0 else inner[::-1]
        order.extend((value,) + rest for rest in steps)
    return order


def ring_order(mesh):
    names = tuple(mesh.axis_names)
    count = mesh.shape["seq"]
    where = [0] * len(names)
    members = []
    for index in range(count):
        where[names.index("seq")] = index
        members.append(mesh.devices[tuple(where)])
    try:
        coords = np.array([list(dev.coords) + [int(getattr(dev, "core_on_chip", 0))] for dev in members])
    except Exception:
        return list(range(count))
    varying = [k for k in range(coords.shape[1]) if len(set(coords[:, k].tolist())) > 1]
    sizes = [len(set(coords[:, k].tolist())) for k in varying]
    if int(np.prod(sizes)) != count:
        return list(range(count))
    lowest = coords[:, varying].min(axis=0)
    lookup = {tuple((coords[i, varying] - lowest).tolist()): i for i in range(count)}
    if len(lookup) != count:
        return list(range(count))
    pairs = [k for k in range(len(sizes)) if sizes[k] == 2]
    if pairs:
        pivot = pairs[-1]
        rest = [sizes[k] for k in range(len(sizes)) if k != pivot]
        path = snake(rest)
        order = []
        for value, steps in ((0, path), (1, path[::-1])):
            for point in steps:
                full = list(point)
                full.insert(pivot, value)
                order.append(full)
    else:
        order = [list(point) for point in snake(sizes)]
    return [lookup[tuple(point)] for point in order]


def shift(value, axis, size, step):
    return lax.ppermute(value, axis, [(a, (a + step) % size) for a in range(size)])


def gather_pairs(value, axis, size, me):
    out = jnp.zeros((size,) + value.shape, value.dtype)
    out = lax.dynamic_update_index_in_dim(out, value, me, 0)
    for step in range(1, size):
        got = shift(value, axis, size, step)
        out = lax.dynamic_update_index_in_dim(out, got, (me - step) % size, 0)
    return out


def scatter_pairs(partial, axis, size, me):
    mine = lax.dynamic_index_in_dim(partial, me, 0, keepdims=False)
    for step in range(1, size):
        send = lax.dynamic_index_in_dim(partial, (me + step) % size, 0, keepdims=False)
        mine = mine + shift(send, axis, size, step)
    return mine


def sum_pairs(value, axis, size):
    total = value
    for step in range(1, size):
        total = total + shift(value, axis, size, step)
    return total


def ring_gather(value, ring, me):
    count = len(ring)
    places = [0] * count
    for k, member in enumerate(ring):
        places[member] = k
    ring_table = jnp.array(ring, jnp.int32)
    here = jnp.array(places, jnp.int32)[me]
    forward = [(ring[k], ring[(k + 1) % count]) for k in range(count)]
    backward = [(ring[(k + 1) % count], ring[k]) for k in range(count)]
    rows = value.shape[0]
    half_rows = rows // 2
    out = jnp.zeros((count,) + value.shape, value.dtype)
    out = lax.dynamic_update_slice(out, value[None], (me, 0, 0))
    ahead, behind = value[:half_rows], value[half_rows:]
    for step in range(1, count):
        ahead = lax.ppermute(ahead, "seq", forward)
        behind = lax.ppermute(behind, "seq", backward)
        source_a = ring_table[(here - step) % count]
        source_b = ring_table[(here + step) % count]
        out = lax.dynamic_update_slice(out, ahead[None], (source_a, 0, 0))
        out = lax.dynamic_update_slice(out, behind[None], (source_b, half_rows, 0))
    return out.reshape((count * rows,) + value.shape[1:])


def shards(
    ring,
    inputs,
    cotangent,
    pre_attention,
    post_attention,
    pre_feedforward,
    post_feedforward,
    query_weight,
    key_matrix,
    value_matrix,
    output_weight,
    gate_weight,
    up_weight,
    down_weight,
    adapter_down,
    adapter_up,
    prefix_lengths,
    adapter_choice,
):
    groups = lax.axis_size("dp")
    parts = lax.axis_size("mp")
    blocks = lax.axis_size("seq")
    quarters = groups * parts
    own = lax.axis_index("dp")
    part = lax.axis_index("mp")
    quarter = part * groups + own
    rows = inputs.shape[2]
    length = rows * blocks
    positions = lax.axis_index("seq") * rows + jnp.arange(rows, dtype=jnp.int32)
    key_positions = jnp.arange(length, dtype=jnp.int32)
    cosine_table, sine_table = angles(positions)
    query_width = QUERY_HEADS_COUNT * HEAD_SIZE
    key_span_width = KEY_VALUE_HEADS * HEAD_SIZE
    query_local = query_width // quarters
    key_local = key_span_width // quarters
    hidden_local = FF // quarters
    half = MODEL_WIDTH // parts
    head_groups = QUERY_HEADS_COUNT // KEY_VALUE_HEADS
    query_heads = query_local // HEAD_SIZE
    key_heads = key_local // HEAD_SIZE
    row_block = MODEL_WIDTH // (groups * blocks)
    scale = HEAD_SIZE ** (-0.5)
    in_output = 3 * MODEL_WIDTH + quarter * query_local
    in_gate = 3 * MODEL_WIDTH + query_width
    in_up = 4 * MODEL_WIDTH + query_width
    in_down = 5 * MODEL_WIDTH + query_width + quarter * hidden_local
    out_query = quarter * query_local
    out_key = query_width + quarter * key_local
    out_value = query_width + key_span_width + quarter * key_local
    out_output = query_width + 2 * key_span_width
    out_gate = query_width + 2 * key_span_width + MODEL_WIDTH + quarter * hidden_local
    out_up = query_width + 2 * key_span_width + MODEL_WIDTH + FF + quarter * hidden_local
    out_down = query_width + 2 * key_span_width + MODEL_WIDTH + 2 * FF
    tokens = groups * rows
    down_widths = (MODEL_WIDTH, MODEL_WIDTH, MODEL_WIDTH, query_width, MODEL_WIDTH, MODEL_WIDTH, FF)
    up_widths = (query_width, key_span_width, key_span_width, MODEL_WIDTH, FF, FF, MODEL_WIDTH)

    def settle(own_down, own_up, choices_now):
        inner = blocks * parts
        down_chunk = own_down.shape[-1] // (groups * inner)
        up_chunk = own_up.shape[-1] // (groups * inner)
        both = jnp.concatenate(
            [
                own_down.reshape(-1, groups, inner, down_chunk),
                own_up.reshape(-1, groups, inner, up_chunk),
            ],
            axis=-1,
        )
        reduced = lax.psum_scatter(both, ("seq", "mp"), scatter_dimension=2, tiled=True)[:, :, 0]
        reduced = jnp.swapaxes(reduced, 0, 1)
        mine = lax.dynamic_update_index_in_dim(
            jnp.zeros_like(reduced), lax.dynamic_index_in_dim(reduced, own, 0, keepdims=False), own, 0
        )
        for step in range(1, groups):
            send = lax.dynamic_index_in_dim(reduced, (own + step) % groups, 0, keepdims=False)
            got = shift(send, "dp", groups, step)
            mine = lax.dynamic_update_index_in_dim(mine, got, (own - step) % groups, 0)
        flat = lax.axis_index(("dp", "seq", "mp"))
        down_part = spread(
            mine[:, :, :down_chunk], choices_now, down_widths, adapter_down.shape[0], flat * down_chunk
        )
        up_part = spread(
            mine[:, :, down_chunk:], choices_now, up_widths, adapter_up.shape[0], flat * up_chunk
        )
        return down_part, up_part

    def to_owner(partial):
        return sum_pairs(scatter_pairs(partial, "dp", groups, own), "mp", parts)

    def permute(value):
        lead = value.shape[:-1]
        moved = value.reshape(lead + (groups, blocks, row_block))
        return jnp.swapaxes(moved, -3, -2).reshape(lead + (MODEL_WIDTH,))

    def unpermute(value):
        lead = value.shape[:-1]
        moved = value.reshape(lead + (blocks, groups, row_block))
        return jnp.swapaxes(moved, -3, -2).reshape(lead + (MODEL_WIDTH,))

    def column_block(weight, index):
        split = weight.reshape(weight.shape[0], groups, -1)
        return lax.dynamic_index_in_dim(split, index, 1, keepdims=False)

    def row_sub(weight, index):
        split = weight.reshape(groups, -1, weight.shape[1])
        return lax.dynamic_index_in_dim(split, index, 0, keepdims=False).T

    column_set = (query_weight, key_matrix, value_matrix)
    row_set = (output_weight,)
    ffw_columns = (gate_weight, up_weight)
    ffw_rows = (down_weight,)

    def swapped(columns, rows_in):
        def block(index):
            return jnp.concatenate(
                [column_block(w, index) for w in columns] + [row_sub(w, index) for w in rows_in], axis=1
            )

        mine = block(own)
        out = lax.dynamic_update_index_in_dim(jnp.zeros((groups,) + mine.shape, mine.dtype), mine, own, 0)
        for step in range(1, groups):
            got = shift(block((own + step) % groups), "dp", groups, step)
            out = lax.dynamic_update_index_in_dim(out, got, (own - step) % groups, 0)
        return out.reshape(-1, out.shape[-1])

    seq_index = lax.axis_index("seq")
    attention_full = ring_gather(swapped(column_set, row_set), ring, seq_index)
    ffw_full = ring_gather(swapped(ffw_columns, ffw_rows), ring, seq_index)
    cut = [0, query_local, key_local, key_local, query_local]
    edges = np.cumsum(cut).tolist()
    query_full = attention_full[:, edges[0] : edges[1]]
    key_full = attention_full[:, edges[1] : edges[2]]
    value_full = attention_full[:, edges[2] : edges[3]]
    output_full = attention_full[:, edges[3] : edges[4]]
    gate_full = ffw_full[:, :hidden_local]
    up_full = ffw_full[:, hidden_local : 2 * hidden_local]
    down_full = ffw_full[:, 2 * hidden_local :]

    sources_all = jnp.swapaxes(gather_pairs(inputs[:, 0], "dp", groups, own), 0, 1)
    prefix_all = gather_pairs(prefix_lengths[:, 0], "dp", groups, own).T
    choices = jnp.swapaxes(gather_pairs(adapter_choice[:, 0], "dp", groups, own), 0, 1)

    def column_forward(inputs_low, weight, down_part, up_part):
        main = jnp.dot(permute(inputs_low).reshape(tokens, MODEL_WIDTH), weight, preferred_element_type=WIDE)
        inner = jnp.einsum("etd,erd->etr", inputs_low, down_part, preferred_element_type=WIDE).astype(NARROW)
        low = jnp.einsum("etr,ero->eto", inner, up_part, preferred_element_type=WIDE)
        return (main.reshape(groups, rows, -1) + low, inner)

    def row_forward(inputs_low, weight, down_part, up_own):
        width = inputs_low.shape[-1]
        main_part = jnp.einsum(
            "tq,dq->td", inputs_low.reshape(tokens, width), weight, preferred_element_type=WIDE
        )
        inner_part = jnp.einsum("etq,erq->etr", inputs_low, down_part, preferred_element_type=WIDE)
        both = jnp.concatenate([main_part.reshape(groups, rows, MODEL_WIDTH), inner_part], axis=-1)
        both = to_owner(both)
        main = unpermute(both[:, :MODEL_WIDTH])
        inner_low = both[:, MODEL_WIDTH:].astype(NARROW)
        return (main + jnp.dot(inner_low, up_own, preferred_element_type=WIDE), inner_low)

    def column_back(grad_out, weight, down_part, up_part, inputs_low, inner_low):
        inner_grad = jnp.einsum("eto,ero->etr", grad_out, up_part, preferred_element_type=WIDE)
        width = grad_out.shape[-1]
        back = jnp.einsum("to,do->td", grad_out.reshape(tokens, width), weight, preferred_element_type=WIDE)
        back = unpermute(back.reshape(groups, rows, MODEL_WIDTH))
        back = back + jnp.einsum("etr,erd->etd", inner_grad, down_part.astype(WIDE), precision=HIGH)
        down_grad = jnp.einsum("etr,etd->erd", inner_grad, inputs_low.astype(WIDE), precision=HIGH)
        up_grad = jnp.einsum("etr,eto->ero", inner_low, grad_out, preferred_element_type=WIDE)
        return (back, down_grad, up_grad)

    def row_back(grad_all, grad_own, weight, down_part, up_part, inputs_low, inner_own):
        inner_grad = jnp.einsum("etd,erd->etr", grad_all, up_part, preferred_element_type=WIDE)
        back = jnp.einsum(
            "td,dq->tq", permute(grad_all).reshape(tokens, MODEL_WIDTH), weight, preferred_element_type=WIDE
        )
        back = back.reshape(groups, rows, -1)
        back = back + jnp.einsum("etr,erq->etq", inner_grad, down_part.astype(WIDE), precision=HIGH)
        down_grad = jnp.einsum("etr,etq->erq", inner_grad, inputs_low.astype(WIDE), precision=HIGH)
        own_columns = lax.dynamic_slice_in_dim(grad_own, part * half, half, 1)
        up_grad = jnp.einsum("tr,tc->rc", inner_own, own_columns, preferred_element_type=WIDE)
        return (back, down_grad, up_grad)

    down_list = []
    up_list = []
    results = []
    input_grads = []
    for batch in range(inputs.shape[0]):
        slots = choices[batch]
        own_slots = adapter_choice[batch, 0]
        prefix_length = prefix_all[batch]
        down_query = picks(adapter_down, slots[:, 0], 0, MODEL_WIDTH)
        down_key = picks(adapter_down, slots[:, 1], MODEL_WIDTH, MODEL_WIDTH)
        down_value = picks(adapter_down, slots[:, 2], 2 * MODEL_WIDTH, MODEL_WIDTH)
        down_output = picks(adapter_down, slots[:, 3], in_output, query_local)
        down_gate = picks(adapter_down, slots[:, 4], in_gate, MODEL_WIDTH)
        down_up = picks(adapter_down, slots[:, 5], in_up, MODEL_WIDTH)
        down_down = picks(adapter_down, slots[:, 6], in_down, hidden_local)
        up_query = picks(adapter_up, slots[:, 0], out_query, query_local)
        up_key = picks(adapter_up, slots[:, 1], out_key, key_local)
        up_value = picks(adapter_up, slots[:, 2], out_value, key_local)
        up_output = picks(adapter_up, slots[:, 3], out_output, MODEL_WIDTH)
        up_gate = picks(adapter_up, slots[:, 4], out_gate, hidden_local)
        up_upper = picks(adapter_up, slots[:, 5], out_up, hidden_local)
        up_down = picks(adapter_up, slots[:, 6], out_down, MODEL_WIDTH)
        up_output_own = pick(adapter_up, own_slots[3], out_output, MODEL_WIDTH)
        up_down_own = pick(adapter_up, own_slots[6], out_down, MODEL_WIDTH)

        source = inputs[batch, 0].astype(WIDE)
        normed = normalize(sources_all[batch].astype(WIDE), pre_attention).astype(NARROW)
        query, inner_query = column_forward(normed, query_full, down_query, up_query)
        key_rows, inner_key = column_forward(normed, key_full, down_key, up_key)
        value_rows, inner_value = column_forward(normed, value_full, down_value, up_value)
        rotated_query = apply_rotation(
            query.reshape(groups, rows, query_heads, HEAD_SIZE), cosine_table, sine_table
        ).astype(NARROW)
        rotated_keys = (
            apply_rotation(key_rows.reshape(groups, rows, key_heads, HEAD_SIZE), cosine_table, sine_table)
            .astype(NARROW)
            .reshape(groups, rows, key_local)
        )
        values_low = value_rows.astype(NARROW)
        both_all = lax.all_gather(jnp.stack([rotated_keys, values_low]), "seq", axis=2, tiled=True)
        keys_three = both_all[0].reshape(groups, length, key_heads, HEAD_SIZE)
        values_three = both_all[1].reshape(groups, length, key_heads, HEAD_SIZE)
        query_four = rotated_query.reshape(groups, rows, key_heads, head_groups, HEAD_SIZE)
        visible = (key_positions[None, None, :] <= positions[None, :, None]) | (
            key_positions[None, None, :] < prefix_length[:, None, None]
        )
        visible = visible[:, None, None]
        raw = (
            jnp.einsum("etkgd,eskd->ekgts", query_four, keys_three, preferred_element_type=WIDE)
            * scale
        )
        masked = jnp.where(visible, SOFT_CAP * jnp.tanh(raw / SOFT_CAP), -1e30)
        top = jnp.max(masked, axis=-1, keepdims=True)
        expo = jnp.exp(masked - top)
        total = jnp.sum(expo, axis=-1, keepdims=True)
        log_total = top + jnp.log(total)
        prob_low = (expo / total).astype(NARROW)
        head_stack = jnp.einsum(
            "ekgts,eskd->etkgd", prob_low, values_three, preferred_element_type=WIDE
        )
        head_stack = head_stack.reshape(groups, rows, query_local).astype(NARROW)
        attention_out, inner_output = row_forward(head_stack, output_full, down_output, up_output_own)
        middle = source + normalize(attention_out, post_attention)
        normed_ffw_own = normalize(middle, pre_feedforward).astype(NARROW)
        normed_ffw = gather_pairs(normed_ffw_own, "dp", groups, own)
        gate, inner_gate = column_forward(normed_ffw, gate_full, down_gate, up_gate)
        upper, inner_upper = column_forward(normed_ffw, up_full, down_up, up_upper)
        hidden = activate(gate, upper).astype(NARROW)
        ffw_out, inner_down = row_forward(hidden, down_full, down_down, up_down_own)
        results.append((middle + normalize(ffw_out, post_feedforward)).astype(NARROW))

        grad_down = jnp.zeros((groups,) + adapter_down.shape[1:], WIDE)
        grad_up = jnp.zeros((groups,) + adapter_up.shape[1:], WIDE)
        seed_grad = cotangent[batch, 0].astype(WIDE)
        grad_ffw_own = normalize_back(ffw_out, post_feedforward, seed_grad).astype(NARROW)
        grad_ffw = gather_pairs(grad_ffw_own, "dp", groups, own)
        grad_hidden, piece_down, piece_up = row_back(
            grad_ffw, grad_ffw_own, down_full, down_down, up_down, hidden, inner_down
        )
        grad_down = place(grad_down, piece_down, in_down)
        grad_up = place_own(grad_up, piece_up, own, out_down + part * half)
        pull = jax.vjp(activate, gate, upper)[1]
        grad_gate, grad_upper = pull(grad_hidden)
        grad_gate = grad_gate.astype(NARROW)
        grad_upper = grad_upper.astype(NARROW)
        back_gate, piece_down, piece_up = column_back(
            grad_gate, gate_full, down_gate, up_gate, normed_ffw, inner_gate
        )
        grad_down = place(grad_down, piece_down, in_gate)
        grad_up = place(grad_up, piece_up, out_gate)
        back_upper, piece_down, piece_up = column_back(
            grad_upper, up_full, down_up, up_upper, normed_ffw, inner_upper
        )
        grad_down = place(grad_down, piece_down, in_up)
        grad_up = place(grad_up, piece_up, out_up)
        grad_normed_ffw = to_owner(back_gate + back_upper)
        grad_middle = seed_grad + normalize_back(middle, pre_feedforward, grad_normed_ffw)
        grad_attention_own = normalize_back(attention_out, post_attention, grad_middle).astype(NARROW)
        grad_attention = gather_pairs(grad_attention_own, "dp", groups, own)
        grad_heads, piece_down, piece_up = row_back(
            grad_attention,
            grad_attention_own,
            output_full,
            down_output,
            up_output,
            head_stack,
            inner_output,
        )
        grad_down = place(grad_down, piece_down, in_output)
        grad_up = place_own(grad_up, piece_up, own, out_output + part * half)
        grad_heads_four = grad_heads.astype(NARROW).reshape(groups, rows, key_heads, head_groups, HEAD_SIZE)
        prob = jnp.exp(masked - log_total)
        grad_prob = jnp.einsum(
            "etkgd,eskd->ekgts", grad_heads_four, values_three, preferred_element_type=WIDE
        )
        grad_capped = prob * (grad_prob - jnp.sum(prob * grad_prob, axis=-1, keepdims=True))
        bend = jnp.tanh(raw / SOFT_CAP)
        grad_raw = (grad_capped * (1.0 - bend * bend)).astype(NARROW)
        grad_query_rot = (
            jnp.einsum("ekgts,eskd->etkgd", grad_raw, keys_three, preferred_element_type=WIDE) * scale
        )
        grad_key_part = (
            jnp.einsum("ekgts,etkgd->eskd", grad_raw, query_four, preferred_element_type=WIDE) * scale
        )
        grad_value_part = jnp.einsum(
            "ekgts,etkgd->eskd", prob_low, grad_heads_four, preferred_element_type=WIDE
        )
        both_grad = lax.psum_scatter(
            jnp.stack(
                [
                    grad_key_part.reshape(groups, length, key_local),
                    grad_value_part.reshape(groups, length, key_local),
                ]
            ),
            "seq",
            scatter_dimension=2,
            tiled=True,
        )
        key_grad, value_grad = both_grad[0], both_grad[1]
        grad_query = (
            rotate_back(
                grad_query_rot.reshape(groups, rows, query_heads, HEAD_SIZE), cosine_table, sine_table
            )
            .reshape(groups, rows, query_local)
            .astype(NARROW)
        )
        grad_key = (
            rotate_back(key_grad.reshape(groups, rows, key_heads, HEAD_SIZE), cosine_table, sine_table)
            .reshape(groups, rows, key_local)
            .astype(NARROW)
        )
        grad_value = value_grad.astype(NARROW)
        back_query, piece_down, piece_up = column_back(
            grad_query, query_full, down_query, up_query, normed, inner_query
        )
        grad_down = place(grad_down, piece_down, 0)
        grad_up = place(grad_up, piece_up, out_query)
        back_key, piece_down, piece_up = column_back(
            grad_key, key_full, down_key, up_key, normed, inner_key
        )
        grad_down = place(grad_down, piece_down, MODEL_WIDTH)
        grad_up = place(grad_up, piece_up, out_key)
        back_value, piece_down, piece_up = column_back(
            grad_value, value_full, down_value, up_value, normed, inner_value
        )
        grad_down = place(grad_down, piece_down, 2 * MODEL_WIDTH)
        grad_up = place(grad_up, piece_up, out_value)
        grad_normed = to_owner(back_query + back_key + back_value)
        own_down = scatter_pairs(grad_down, "dp", groups, own)
        own_up = scatter_pairs(grad_up, "dp", groups, own)
        down_part, up_part = settle(own_down, own_up, slots)
        down_list.append(down_part)
        up_list.append(up_part)
        input_grads.append(
            (grad_middle + normalize_back(source, pre_attention, grad_normed)).astype(NARROW)
        )
    down_total = down_list[0]
    up_total = up_list[0]
    for extra in range(1, len(down_list)):
        down_total = down_total + down_list[extra]
        up_total = up_total + up_list[extra]
    outputs = jnp.stack(results)[:, None]
    input_gradient = jnp.stack(input_grads)[:, None]
    return (outputs, input_gradient, down_total, up_total)


def solution(mesh):
    ring = ring_order(mesh)

    def body(*args):
        return shards(ring, *args)

    return jax.shard_map(
        body,
        mesh=mesh,
        in_specs=(
            P(None, "dp", "seq", None),
            P(None, "dp", "seq", None),
            P(),
            P(),
            P(),
            P(),
            P(("dp", "seq"), "mp"),
            P(("dp", "seq"), "mp"),
            P(("dp", "seq"), "mp"),
            P("mp", ("dp", "seq")),
            P(("dp", "seq"), "mp"),
            P(("dp", "seq"), "mp"),
            P("mp", ("dp", "seq")),
            P(),
            P(),
            P(None, "dp"),
            P(None, "dp", None),
        ),
        out_specs=(
            P(None, "dp", "seq", None),
            P(None, "dp", "seq", None),
            P(None, None, ("dp", "seq", "mp")),
            P(None, None, ("dp", "seq", "mp")),
        ),
        check_vma=False,
    )
```

```python
import numpy as np
import jax
import jax.numpy as jnp
from jax import lax
from jax.sharding import PartitionSpec as P

MODEL_WIDTH = 2304
QUERY_HEADS_COUNT = 8
KEY_VALUE_HEADS = 4
HEAD_SIZE = 256
FF = 9216


HIGH = lax.Precision.HIGHEST
EPSILON = 1e-06
SOFT_CAP = 50.0
WIDE = jnp.float32
NARROW = jnp.bfloat16


def normalize(value, gain):
    factor = lax.rsqrt(jnp.mean(value * value, axis=-1, keepdims=True) + EPSILON)
    return value * factor * gain


def normalize_back(value, gain, upstream):
    factor = lax.rsqrt(jnp.mean(value * value, axis=-1, keepdims=True) + EPSILON)
    scaled = upstream * gain
    inner = jnp.mean(value * scaled, axis=-1, keepdims=True)
    return factor * scaled - value * (factor * factor * factor) * inner


def angles(positions):
    half = HEAD_SIZE // 2
    rates = 10000.0 ** (-(jnp.arange(half, dtype=WIDE) * 2.0) / HEAD_SIZE)
    turns = positions.astype(WIDE)[:, None] * rates[None, :]
    return (jnp.cos(turns)[:, None, :], jnp.sin(turns)[:, None, :])


def apply_rotation(head_stack, cosine_table, sine_table):
    half = HEAD_SIZE // 2
    first = head_stack[..., :half]
    second = head_stack[..., half:]
    return jnp.concatenate(
        [first * cosine_table - second * sine_table, second * cosine_table + first * sine_table],
        axis=-1,
    )


def rotate_back(grads, cosine_table, sine_table):
    half = HEAD_SIZE // 2
    first = grads[..., :half]
    second = grads[..., half:]
    return jnp.concatenate(
        [first * cosine_table + second * sine_table, second * cosine_table - first * sine_table],
        axis=-1,
    )


def pick(table, index, start_index, size):
    window = lax.dynamic_slice_in_dim(table, start_index, size, axis=2)
    hit = jnp.arange(table.shape[0], dtype=jnp.int32) == index
    return jnp.sum(jnp.where(hit[:, None, None], window.astype(WIDE), 0.0), axis=0).astype(table.dtype)


def picks(table, slots, start_index, size):
    return jnp.stack([pick(table, slots[e], start_index, size) for e in range(slots.shape[0])])


def place(total, piece, start_index):
    return lax.dynamic_update_slice(total, piece, (0, 0, start_index))


def place_own(total, piece, own, start_index):
    return lax.dynamic_update_slice(total, piece[None], (own, 0, start_index))


def activate(gate_value, up_value):
    return jax.nn.gelu(gate_value, approximate=True) * up_value


def segment_of(columns, widths):
    seg = jnp.zeros(columns.shape, jnp.int32)
    edge = 0
    for width in widths[:-1]:
        edge += width
        seg = seg + (columns >= edge).astype(jnp.int32)
    return seg


def spread(compact, choices, widths, adapters, start):
    columns = start + jnp.arange(compact.shape[-1], dtype=jnp.int32)
    seg = segment_of(columns, widths)
    chosen = jnp.zeros((choices.shape[0], compact.shape[-1]), jnp.int32)
    for index in range(len(widths)):
        chosen = chosen + jnp.where(seg == index, choices[:, index : index + 1], 0)
    hits = chosen[None] == jnp.arange(adapters, dtype=jnp.int32)[:, None, None]
    picked = jnp.where(hits[:, :, None, :], compact[None], 0.0)
    return jnp.sum(picked, axis=1)


def snake(sizes):
    if not sizes:
        return [()]
    inner = snake(sizes[1:])
    order = []
    for value in range(sizes[0]):
        steps = inner if value % 2 == 0 else inner[::-1]
        order.extend((value,) + rest for rest in steps)
    return order


def ring_order(mesh):
    names = tuple(mesh.axis_names)
    count = mesh.shape["seq"]
    where = [0] * len(names)
    members = []
    for index in range(count):
        where[names.index("seq")] = index
        members.append(mesh.devices[tuple(where)])
    try:
        coords = np.array([list(dev.coords) + [int(getattr(dev, "core_on_chip", 0))] for dev in members])
    except Exception:
        return list(range(count))
    varying = [k for k in range(coords.shape[1]) if len(set(coords[:, k].tolist())) > 1]
    sizes = [len(set(coords[:, k].tolist())) for k in varying]
    if int(np.prod(sizes)) != count:
        return list(range(count))
    lowest = coords[:, varying].min(axis=0)
    lookup = {tuple((coords[i, varying] - lowest).tolist()): i for i in range(count)}
    if len(lookup) != count:
        return list(range(count))
    pairs = [k for k in range(len(sizes)) if sizes[k] == 2]
    if pairs:
        pivot = pairs[-1]
        rest = [sizes[k] for k in range(len(sizes)) if k != pivot]
        path = snake(rest)
        order = []
        for value, steps in ((0, path), (1, path[::-1])):
            for point in steps:
                full = list(point)
                full.insert(pivot, value)
                order.append(full)
    else:
        order = [list(point) for point in snake(sizes)]
    return [lookup[tuple(point)] for point in order]


def wrap(index, step, size):
    return jnp.array([(a + step) % size for a in range(size)], jnp.int32)[index]


def shift(value, axis, size, step):
    return lax.ppermute(value, axis, [(a, (a + step) % size) for a in range(size)])


def gather_pairs(value, axis, size, me):
    out = jnp.zeros((size,) + value.shape, value.dtype)
    out = lax.dynamic_update_index_in_dim(out, value, me, 0)
    for step in range(1, size):
        got = shift(value, axis, size, step)
        out = lax.dynamic_update_index_in_dim(out, got, wrap(me, -step, size), 0)
    return out


def scatter_pairs(partial, axis, size, me):
    mine = lax.dynamic_index_in_dim(partial, me, 0, keepdims=False)
    for step in range(1, size):
        send = lax.dynamic_index_in_dim(partial, wrap(me, step, size), 0, keepdims=False)
        mine = mine + shift(send, axis, size, step)
    return mine


def sum_pairs(value, axis, size):
    total = value
    for step in range(1, size):
        total = total + shift(value, axis, size, step)
    return total


def ring_gather(value, ring, me):
    count = len(ring)
    places = [0] * count
    for k, member in enumerate(ring):
        places[member] = k
    ahead_from = jnp.array(
        [[ring[(places[j] - s) % count] for s in range(count)] for j in range(count)], jnp.int32
    )[me]
    behind_from = jnp.array(
        [[ring[(places[j] + s) % count] for s in range(count)] for j in range(count)], jnp.int32
    )[me]
    forward = [(ring[k], ring[(k + 1) % count]) for k in range(count)]
    backward = [(ring[(k + 1) % count], ring[k]) for k in range(count)]
    rows = value.shape[0]
    half_rows = rows // 2
    out = jnp.zeros((count,) + value.shape, value.dtype)
    out = lax.dynamic_update_slice(out, value[None], (me, 0, 0))
    ahead, behind = value[:half_rows], value[half_rows:]
    for step in range(1, count):
        ahead = lax.ppermute(ahead, "seq", forward)
        behind = lax.ppermute(behind, "seq", backward)
        source_a = ahead_from[step]
        source_b = behind_from[step]
        out = lax.dynamic_update_slice(out, ahead[None], (source_a, 0, 0))
        out = lax.dynamic_update_slice(out, behind[None], (source_b, half_rows, 0))
    return out.reshape((count * rows,) + value.shape[1:])


def shards(
    ring,
    inputs,
    cotangent,
    pre_attention,
    post_attention,
    pre_feedforward,
    post_feedforward,
    query_weight,
    key_matrix,
    value_matrix,
    output_weight,
    gate_weight,
    up_weight,
    down_weight,
    adapter_down,
    adapter_up,
    prefix_lengths,
    adapter_choice,
):
    groups = lax.axis_size("dp")
    parts = lax.axis_size("mp")
    blocks = lax.axis_size("seq")
    quarters = groups * parts
    own = lax.axis_index("dp")
    part = lax.axis_index("mp")
    quarter = part * groups + own
    rows = inputs.shape[2]
    length = rows * blocks
    positions = lax.axis_index("seq") * rows + jnp.arange(rows, dtype=jnp.int32)
    key_positions = jnp.arange(length, dtype=jnp.int32)
    cosine_table, sine_table = angles(positions)
    query_width = QUERY_HEADS_COUNT * HEAD_SIZE
    key_span_width = KEY_VALUE_HEADS * HEAD_SIZE
    query_local = query_width // quarters
    key_local = key_span_width // quarters
    hidden_local = FF // quarters
    half = MODEL_WIDTH // parts
    head_groups = QUERY_HEADS_COUNT // KEY_VALUE_HEADS
    query_heads = query_local // HEAD_SIZE
    key_heads = key_local // HEAD_SIZE
    row_block = MODEL_WIDTH // (groups * blocks)
    scale = HEAD_SIZE ** (-0.5)
    in_output = 3 * MODEL_WIDTH + quarter * query_local
    in_gate = 3 * MODEL_WIDTH + query_width
    in_up = 4 * MODEL_WIDTH + query_width
    in_down = 5 * MODEL_WIDTH + query_width + quarter * hidden_local
    out_query = quarter * query_local
    out_key = query_width + quarter * key_local
    out_value = query_width + key_span_width + quarter * key_local
    out_output = query_width + 2 * key_span_width
    out_gate = query_width + 2 * key_span_width + MODEL_WIDTH + quarter * hidden_local
    out_up = query_width + 2 * key_span_width + MODEL_WIDTH + FF + quarter * hidden_local
    out_down = query_width + 2 * key_span_width + MODEL_WIDTH + 2 * FF
    tokens = groups * rows
    down_widths = (MODEL_WIDTH, MODEL_WIDTH, MODEL_WIDTH, query_width, MODEL_WIDTH, MODEL_WIDTH, FF)
    up_widths = (query_width, key_span_width, key_span_width, MODEL_WIDTH, FF, FF, MODEL_WIDTH)

    def settle(own_down, own_up, choices_now):
        inner = blocks * parts
        down_chunk = own_down.shape[-1] // (groups * inner)
        up_chunk = own_up.shape[-1] // (groups * inner)
        both = jnp.concatenate(
            [
                own_down.reshape(-1, groups, inner, down_chunk),
                own_up.reshape(-1, groups, inner, up_chunk),
            ],
            axis=-1,
        )
        reduced = lax.psum_scatter(both, ("seq", "mp"), scatter_dimension=2, tiled=True)[:, :, 0]
        reduced = jnp.swapaxes(reduced, 0, 1)
        mine = lax.dynamic_update_index_in_dim(
            jnp.zeros_like(reduced), lax.dynamic_index_in_dim(reduced, own, 0, keepdims=False), own, 0
        )
        for step in range(1, groups):
            send = lax.dynamic_index_in_dim(reduced, wrap(own, step, groups), 0, keepdims=False)
            got = shift(send, "dp", groups, step)
            mine = lax.dynamic_update_index_in_dim(mine, got, wrap(own, -step, groups), 0)
        flat = lax.axis_index(("dp", "seq", "mp"))
        down_part = spread(
            mine[:, :, :down_chunk], choices_now, down_widths, adapter_down.shape[0], flat * down_chunk
        )
        up_part = spread(
            mine[:, :, down_chunk:], choices_now, up_widths, adapter_up.shape[0], flat * up_chunk
        )
        return down_part, up_part

    def to_owner(partial):
        return sum_pairs(scatter_pairs(partial, "dp", groups, own), "mp", parts)

    def permute(value):
        lead = value.shape[:-1]
        moved = value.reshape(lead + (groups, blocks, row_block))
        return jnp.swapaxes(moved, -3, -2).reshape(lead + (MODEL_WIDTH,))

    def unpermute(value):
        lead = value.shape[:-1]
        moved = value.reshape(lead + (blocks, groups, row_block))
        return jnp.swapaxes(moved, -3, -2).reshape(lead + (MODEL_WIDTH,))

    def column_block(weight, index):
        split = weight.reshape(weight.shape[0], groups, -1)
        return lax.dynamic_index_in_dim(split, index, 1, keepdims=False)

    def row_sub(weight, index):
        split = weight.reshape(groups, -1, weight.shape[1])
        return lax.dynamic_index_in_dim(split, index, 0, keepdims=False).T

    column_set = (query_weight, key_matrix, value_matrix)
    row_set = (output_weight,)
    ffw_columns = (gate_weight, up_weight)
    ffw_rows = (down_weight,)

    def swapped(columns, rows_in):
        def block(index):
            return jnp.concatenate(
                [column_block(w, index) for w in columns] + [row_sub(w, index) for w in rows_in], axis=1
            )

        mine = block(own)
        out = lax.dynamic_update_index_in_dim(jnp.zeros((groups,) + mine.shape, mine.dtype), mine, own, 0)
        for step in range(1, groups):
            got = shift(block(wrap(own, step, groups)), "dp", groups, step)
            out = lax.dynamic_update_index_in_dim(out, got, wrap(own, -step, groups), 0)
        return out.reshape(-1, out.shape[-1])

    seq_index = lax.axis_index("seq")
    attention_full = ring_gather(swapped(column_set, row_set), ring, seq_index)
    ffw_full = ring_gather(swapped(ffw_columns, ffw_rows), ring, seq_index)
    cut = [0, query_local, key_local, key_local, query_local]
    edges = np.cumsum(cut).tolist()
    query_full = attention_full[:, edges[0] : edges[1]]
    key_full = attention_full[:, edges[1] : edges[2]]
    value_full = attention_full[:, edges[2] : edges[3]]
    output_full = attention_full[:, edges[3] : edges[4]]
    gate_full = ffw_full[:, :hidden_local]
    up_full = ffw_full[:, hidden_local : 2 * hidden_local]
    down_full = ffw_full[:, 2 * hidden_local :]

    sources_all = jnp.swapaxes(gather_pairs(inputs[:, 0], "dp", groups, own), 0, 1)
    prefix_all = gather_pairs(prefix_lengths[:, 0], "dp", groups, own).T
    choices = jnp.swapaxes(gather_pairs(adapter_choice[:, 0], "dp", groups, own), 0, 1)

    def column_forward(inputs_low, weight, down_part, up_part):
        main = jnp.dot(permute(inputs_low).reshape(tokens, MODEL_WIDTH), weight, preferred_element_type=WIDE)
        inner = jnp.einsum("etd,erd->etr", inputs_low, down_part, preferred_element_type=WIDE).astype(NARROW)
        low = jnp.einsum("etr,ero->eto", inner, up_part, preferred_element_type=WIDE)
        return (main.reshape(groups, rows, -1) + low, inner)

    def row_forward(inputs_low, weight, down_part, up_own):
        width = inputs_low.shape[-1]
        main_part = jnp.einsum(
            "tq,dq->td", inputs_low.reshape(tokens, width), weight, preferred_element_type=WIDE
        )
        inner_part = jnp.einsum("etq,erq->etr", inputs_low, down_part, preferred_element_type=WIDE)
        both = jnp.concatenate([main_part.reshape(groups, rows, MODEL_WIDTH), inner_part], axis=-1)
        both = to_owner(both)
        main = unpermute(both[:, :MODEL_WIDTH])
        inner_low = both[:, MODEL_WIDTH:].astype(NARROW)
        return (main + jnp.dot(inner_low, up_own, preferred_element_type=WIDE), inner_low)

    def column_back(grad_out, weight, down_part, up_part, inputs_low, inner_low):
        inner_grad = jnp.einsum("eto,ero->etr", grad_out, up_part, preferred_element_type=WIDE)
        width = grad_out.shape[-1]
        back = jnp.einsum("to,do->td", grad_out.reshape(tokens, width), weight, preferred_element_type=WIDE)
        back = unpermute(back.reshape(groups, rows, MODEL_WIDTH))
        back = back + jnp.einsum("etr,erd->etd", inner_grad, down_part.astype(WIDE), precision=HIGH)
        down_grad = jnp.einsum("etr,etd->erd", inner_grad, inputs_low.astype(WIDE), precision=HIGH)
        up_grad = jnp.einsum("etr,eto->ero", inner_low, grad_out, preferred_element_type=WIDE)
        return (back, down_grad, up_grad)

    def row_back(grad_all, grad_own, weight, down_part, up_part, inputs_low, inner_own):
        inner_grad = jnp.einsum("etd,erd->etr", grad_all, up_part, preferred_element_type=WIDE)
        back = jnp.einsum(
            "td,dq->tq", permute(grad_all).reshape(tokens, MODEL_WIDTH), weight, preferred_element_type=WIDE
        )
        back = back.reshape(groups, rows, -1)
        back = back + jnp.einsum("etr,erq->etq", inner_grad, down_part.astype(WIDE), precision=HIGH)
        down_grad = jnp.einsum("etr,etq->erq", inner_grad, inputs_low.astype(WIDE), precision=HIGH)
        own_columns = lax.dynamic_slice_in_dim(grad_own, part * half, half, 1)
        up_grad = jnp.einsum("tr,tc->rc", inner_own, own_columns, preferred_element_type=WIDE)
        return (back, down_grad, up_grad)

    down_list = []
    up_list = []
    results = []
    input_grads = []
    for batch in range(inputs.shape[0]):
        slots = choices[batch]
        own_slots = adapter_choice[batch, 0]
        prefix_length = prefix_all[batch]
        down_query = picks(adapter_down, slots[:, 0], 0, MODEL_WIDTH)
        down_key = picks(adapter_down, slots[:, 1], MODEL_WIDTH, MODEL_WIDTH)
        down_value = picks(adapter_down, slots[:, 2], 2 * MODEL_WIDTH, MODEL_WIDTH)
        down_output = picks(adapter_down, slots[:, 3], in_output, query_local)
        down_gate = picks(adapter_down, slots[:, 4], in_gate, MODEL_WIDTH)
        down_up = picks(adapter_down, slots[:, 5], in_up, MODEL_WIDTH)
        down_down = picks(adapter_down, slots[:, 6], in_down, hidden_local)
        up_query = picks(adapter_up, slots[:, 0], out_query, query_local)
        up_key = picks(adapter_up, slots[:, 1], out_key, key_local)
        up_value = picks(adapter_up, slots[:, 2], out_value, key_local)
        up_output = picks(adapter_up, slots[:, 3], out_output, MODEL_WIDTH)
        up_gate = picks(adapter_up, slots[:, 4], out_gate, hidden_local)
        up_upper = picks(adapter_up, slots[:, 5], out_up, hidden_local)
        up_down = picks(adapter_up, slots[:, 6], out_down, MODEL_WIDTH)
        up_output_own = pick(adapter_up, own_slots[3], out_output, MODEL_WIDTH)
        up_down_own = pick(adapter_up, own_slots[6], out_down, MODEL_WIDTH)

        source = inputs[batch, 0].astype(WIDE)
        normed = normalize(sources_all[batch].astype(WIDE), pre_attention).astype(NARROW)
        query, inner_query = column_forward(normed, query_full, down_query, up_query)
        key_rows, inner_key = column_forward(normed, key_full, down_key, up_key)
        value_rows, inner_value = column_forward(normed, value_full, down_value, up_value)
        rotated_query = apply_rotation(
            query.reshape(groups, rows, query_heads, HEAD_SIZE), cosine_table, sine_table
        ).astype(NARROW)
        rotated_keys = (
            apply_rotation(key_rows.reshape(groups, rows, key_heads, HEAD_SIZE), cosine_table, sine_table)
            .astype(NARROW)
            .reshape(groups, rows, key_local)
        )
        values_low = value_rows.astype(NARROW)
        both_all = lax.all_gather(jnp.stack([rotated_keys, values_low]), "seq", axis=2, tiled=True)
        keys_three = both_all[0].reshape(groups, length, key_heads, HEAD_SIZE)
        values_three = both_all[1].reshape(groups, length, key_heads, HEAD_SIZE)
        query_four = rotated_query.reshape(groups, rows, key_heads, head_groups, HEAD_SIZE)
        visible = (key_positions[None, None, :] <= positions[None, :, None]) | (
            key_positions[None, None, :] < prefix_length[:, None, None]
        )
        visible = visible[:, None, None]
        raw = (
            jnp.einsum("etkgd,eskd->ekgts", query_four, keys_three, preferred_element_type=WIDE)
            * scale
        )
        masked = jnp.where(visible, SOFT_CAP * jnp.tanh(raw / SOFT_CAP), -1e30)
        top = jnp.max(masked, axis=-1, keepdims=True)
        expo = jnp.exp(masked - top)
        total = jnp.sum(expo, axis=-1, keepdims=True)
        log_total = top + jnp.log(total)
        prob_low = (expo / total).astype(NARROW)
        head_stack = jnp.einsum(
            "ekgts,eskd->etkgd", prob_low, values_three, preferred_element_type=WIDE
        )
        head_stack = head_stack.reshape(groups, rows, query_local).astype(NARROW)
        attention_out, inner_output = row_forward(head_stack, output_full, down_output, up_output_own)
        middle = source + normalize(attention_out, post_attention)
        normed_ffw_own = normalize(middle, pre_feedforward).astype(NARROW)
        normed_ffw = gather_pairs(normed_ffw_own, "dp", groups, own)
        gate, inner_gate = column_forward(normed_ffw, gate_full, down_gate, up_gate)
        upper, inner_upper = column_forward(normed_ffw, up_full, down_up, up_upper)
        hidden = activate(gate, upper).astype(NARROW)
        ffw_out, inner_down = row_forward(hidden, down_full, down_down, up_down_own)
        results.append((middle + normalize(ffw_out, post_feedforward)).astype(NARROW))

        grad_down = jnp.zeros((groups,) + adapter_down.shape[1:], WIDE)
        grad_up = jnp.zeros((groups,) + adapter_up.shape[1:], WIDE)
        seed_grad = cotangent[batch, 0].astype(WIDE)
        grad_ffw_own = normalize_back(ffw_out, post_feedforward, seed_grad).astype(NARROW)
        grad_ffw = gather_pairs(grad_ffw_own, "dp", groups, own)
        grad_hidden, piece_down, piece_up = row_back(
            grad_ffw, grad_ffw_own, down_full, down_down, up_down, hidden, inner_down
        )
        grad_down = place(grad_down, piece_down, in_down)
        grad_up = place_own(grad_up, piece_up, own, out_down + part * half)
        pull = jax.vjp(activate, gate, upper)[1]
        grad_gate, grad_upper = pull(grad_hidden)
        grad_gate = grad_gate.astype(NARROW)
        grad_upper = grad_upper.astype(NARROW)
        back_gate, piece_down, piece_up = column_back(
            grad_gate, gate_full, down_gate, up_gate, normed_ffw, inner_gate
        )
        grad_down = place(grad_down, piece_down, in_gate)
        grad_up = place(grad_up, piece_up, out_gate)
        back_upper, piece_down, piece_up = column_back(
            grad_upper, up_full, down_up, up_upper, normed_ffw, inner_upper
        )
        grad_down = place(grad_down, piece_down, in_up)
        grad_up = place(grad_up, piece_up, out_up)
        grad_normed_ffw = to_owner(back_gate + back_upper)
        grad_middle = seed_grad + normalize_back(middle, pre_feedforward, grad_normed_ffw)
        grad_attention_own = normalize_back(attention_out, post_attention, grad_middle).astype(NARROW)
        grad_attention = gather_pairs(grad_attention_own, "dp", groups, own)
        grad_heads, piece_down, piece_up = row_back(
            grad_attention,
            grad_attention_own,
            output_full,
            down_output,
            up_output,
            head_stack,
            inner_output,
        )
        grad_down = place(grad_down, piece_down, in_output)
        grad_up = place_own(grad_up, piece_up, own, out_output + part * half)
        grad_heads_four = grad_heads.astype(NARROW).reshape(groups, rows, key_heads, head_groups, HEAD_SIZE)
        prob = jnp.exp(masked - log_total)
        grad_prob = jnp.einsum(
            "etkgd,eskd->ekgts", grad_heads_four, values_three, preferred_element_type=WIDE
        )
        grad_capped = prob * (grad_prob - jnp.sum(prob * grad_prob, axis=-1, keepdims=True))
        bend = jnp.tanh(raw / SOFT_CAP)
        grad_raw = (grad_capped * (1.0 - bend * bend)).astype(NARROW)
        grad_query_rot = (
            jnp.einsum("ekgts,eskd->etkgd", grad_raw, keys_three, preferred_element_type=WIDE) * scale
        )
        grad_key_part = (
            jnp.einsum("ekgts,etkgd->eskd", grad_raw, query_four, preferred_element_type=WIDE) * scale
        )
        grad_value_part = jnp.einsum(
            "ekgts,etkgd->eskd", prob_low, grad_heads_four, preferred_element_type=WIDE
        )
        both_grad = lax.psum_scatter(
            jnp.stack(
                [
                    grad_key_part.reshape(groups, length, key_local),
                    grad_value_part.reshape(groups, length, key_local),
                ]
            ),
            "seq",
            scatter_dimension=2,
            tiled=True,
        )
        key_grad, value_grad = both_grad[0], both_grad[1]
        grad_query = (
            rotate_back(
                grad_query_rot.reshape(groups, rows, query_heads, HEAD_SIZE), cosine_table, sine_table
            )
            .reshape(groups, rows, query_local)
            .astype(NARROW)
        )
        grad_key = (
            rotate_back(key_grad.reshape(groups, rows, key_heads, HEAD_SIZE), cosine_table, sine_table)
            .reshape(groups, rows, key_local)
            .astype(NARROW)
        )
        grad_value = value_grad.astype(NARROW)
        back_query, piece_down, piece_up = column_back(
            grad_query, query_full, down_query, up_query, normed, inner_query
        )
        grad_down = place(grad_down, piece_down, 0)
        grad_up = place(grad_up, piece_up, out_query)
        back_key, piece_down, piece_up = column_back(
            grad_key, key_full, down_key, up_key, normed, inner_key
        )
        grad_down = place(grad_down, piece_down, MODEL_WIDTH)
        grad_up = place(grad_up, piece_up, out_key)
        back_value, piece_down, piece_up = column_back(
            grad_value, value_full, down_value, up_value, normed, inner_value
        )
        grad_down = place(grad_down, piece_down, 2 * MODEL_WIDTH)
        grad_up = place(grad_up, piece_up, out_value)
        grad_normed = to_owner(back_query + back_key + back_value)
        own_down = scatter_pairs(grad_down, "dp", groups, own)
        own_up = scatter_pairs(grad_up, "dp", groups, own)
        down_part, up_part = settle(own_down, own_up, slots)
        down_list.append(down_part)
        up_list.append(up_part)
        input_grads.append(
            (grad_middle + normalize_back(source, pre_attention, grad_normed)).astype(NARROW)
        )
    down_total = down_list[0]
    up_total = up_list[0]
    for extra in range(1, len(down_list)):
        down_total = down_total + down_list[extra]
        up_total = up_total + up_list[extra]
    outputs = jnp.stack(results)[:, None]
    input_gradient = jnp.stack(input_grads)[:, None]
    return (outputs, input_gradient, down_total, up_total)


def solution(mesh):
    ring = ring_order(mesh)

    def body(*args):
        return shards(ring, *args)

    return jax.shard_map(
        body,
        mesh=mesh,
        in_specs=(
            P(None, "dp", "seq", None),
            P(None, "dp", "seq", None),
            P(),
            P(),
            P(),
            P(),
            P(("dp", "seq"), "mp"),
            P(("dp", "seq"), "mp"),
            P(("dp", "seq"), "mp"),
            P("mp", ("dp", "seq")),
            P(("dp", "seq"), "mp"),
            P(("dp", "seq"), "mp"),
            P("mp", ("dp", "seq")),
            P(),
            P(),
            P(None, "dp"),
            P(None, "dp", None),
        ),
        out_specs=(
            P(None, "dp", "seq", None),
            P(None, "dp", "seq", None),
            P(None, None, ("dp", "seq", "mp")),
            P(None, None, ("dp", "seq", "mp")),
        ),
        check_vma=False,
    )
```

```python
import numpy as np
import jax
import jax.numpy as jnp
from jax import lax
from jax.sharding import PartitionSpec as P

MODEL_WIDTH = 2304
QUERY_HEADS_COUNT = 8
KEY_VALUE_HEADS = 4
HEAD_SIZE = 256
FF = 9216


HIGH = lax.Precision.HIGHEST
EPSILON = 1e-06
SOFT_CAP = 50.0
WIDE = jnp.float32
NARROW = jnp.bfloat16


def normalize(value, gain):
    factor = lax.rsqrt(jnp.mean(value * value, axis=-1, keepdims=True) + EPSILON)
    return value * factor * gain


def normalize_back(value, gain, upstream):
    factor = lax.rsqrt(jnp.mean(value * value, axis=-1, keepdims=True) + EPSILON)
    scaled = upstream * gain
    inner = jnp.mean(value * scaled, axis=-1, keepdims=True)
    return factor * scaled - value * (factor * factor * factor) * inner


def angles(positions):
    half = HEAD_SIZE // 2
    rates = 10000.0 ** (-(jnp.arange(half, dtype=WIDE) * 2.0) / HEAD_SIZE)
    turns = positions.astype(WIDE)[:, None] * rates[None, :]
    return (jnp.cos(turns)[:, None, :], jnp.sin(turns)[:, None, :])


def apply_rotation(head_stack, cosine_table, sine_table):
    half = HEAD_SIZE // 2
    first = head_stack[..., :half]
    second = head_stack[..., half:]
    return jnp.concatenate(
        [first * cosine_table - second * sine_table, second * cosine_table + first * sine_table],
        axis=-1,
    )


def rotate_back(grads, cosine_table, sine_table):
    half = HEAD_SIZE // 2
    first = grads[..., :half]
    second = grads[..., half:]
    return jnp.concatenate(
        [first * cosine_table + second * sine_table, second * cosine_table - first * sine_table],
        axis=-1,
    )


def pick(table, index, start_index, size):
    window = lax.dynamic_slice_in_dim(table, start_index, size, axis=2)
    hit = jnp.arange(table.shape[0], dtype=jnp.int32) == index
    return jnp.sum(jnp.where(hit[:, None, None], window.astype(WIDE), 0.0), axis=0).astype(table.dtype)


def picks(table, slots, start_index, size):
    return jnp.stack([pick(table, slots[e], start_index, size) for e in range(slots.shape[0])])


def place(total, piece, start_index):
    return lax.dynamic_update_slice(total, piece, (0, 0, start_index))


def place_own(total, piece, own, start_index):
    return lax.dynamic_update_slice(total, piece[None], (own, 0, start_index))


def activate(gate_value, up_value):
    return jax.nn.gelu(gate_value, approximate=True) * up_value


def segment_of(columns, widths):
    seg = jnp.zeros(columns.shape, jnp.int32)
    edge = 0
    for width in widths[:-1]:
        edge += width
        seg = seg + (columns >= edge).astype(jnp.int32)
    return seg


def spread(compact, choices, widths, adapters, start):
    columns = start + jnp.arange(compact.shape[-1], dtype=jnp.int32)
    seg = segment_of(columns, widths)
    chosen = jnp.zeros((choices.shape[0], compact.shape[-1]), jnp.int32)
    for index in range(len(widths)):
        chosen = chosen + jnp.where(seg == index, choices[:, index : index + 1], 0)
    hits = chosen[None] == jnp.arange(adapters, dtype=jnp.int32)[:, None, None]
    picked = jnp.where(hits[:, :, None, :], compact[None], 0.0)
    return jnp.sum(picked, axis=1)


def snake(sizes):
    if not sizes:
        return [()]
    inner = snake(sizes[1:])
    order = []
    for value in range(sizes[0]):
        steps = inner if value % 2 == 0 else inner[::-1]
        order.extend((value,) + rest for rest in steps)
    return order


def ring_order(mesh):
    names = tuple(mesh.axis_names)
    count = mesh.shape["seq"]
    where = [0] * len(names)
    members = []
    for index in range(count):
        where[names.index("seq")] = index
        members.append(mesh.devices[tuple(where)])
    try:
        coords = np.array([list(dev.coords) + [int(getattr(dev, "core_on_chip", 0))] for dev in members])
    except Exception:
        return list(range(count))
    varying = [k for k in range(coords.shape[1]) if len(set(coords[:, k].tolist())) > 1]
    sizes = [len(set(coords[:, k].tolist())) for k in varying]
    if int(np.prod(sizes)) != count:
        return list(range(count))
    lowest = coords[:, varying].min(axis=0)
    lookup = {tuple((coords[i, varying] - lowest).tolist()): i for i in range(count)}
    if len(lookup) != count:
        return list(range(count))
    pairs = [k for k in range(len(sizes)) if sizes[k] == 2]
    if pairs:
        pivot = pairs[-1]
        rest = [sizes[k] for k in range(len(sizes)) if k != pivot]
        path = snake(rest)
        order = []
        for value, steps in ((0, path), (1, path[::-1])):
            for point in steps:
                full = list(point)
                full.insert(pivot, value)
                order.append(full)
    else:
        order = [list(point) for point in snake(sizes)]
    return [lookup[tuple(point)] for point in order]


def wrap(index, step, size):
    return jnp.array([(a + step) % size for a in range(size)], jnp.int32)[index]


def shift(value, axis, size, step):
    return lax.ppermute(value, axis, [(a, (a + step) % size) for a in range(size)])


def gather_pairs(value, axis, size, me):
    out = jnp.zeros((size,) + value.shape, value.dtype)
    out = lax.dynamic_update_index_in_dim(out, value, me, 0)
    for step in range(1, size):
        got = shift(value, axis, size, step)
        out = lax.dynamic_update_index_in_dim(out, got, wrap(me, -step, size), 0)
    return out


def scatter_pairs(partial, axis, size, me):
    mine = lax.dynamic_index_in_dim(partial, me, 0, keepdims=False)
    for step in range(1, size):
        send = lax.dynamic_index_in_dim(partial, wrap(me, step, size), 0, keepdims=False)
        mine = mine + shift(send, axis, size, step)
    return mine


def sum_pairs(value, axis, size):
    total = value
    for step in range(1, size):
        total = total + shift(value, axis, size, step)
    return total


def ring_gather(value, ring, me):
    count = len(ring)
    places = [0] * count
    for k, member in enumerate(ring):
        places[member] = k
    ahead_from = jnp.array(
        [[ring[(places[j] - s) % count] for s in range(count)] for j in range(count)], jnp.int32
    )[me]
    behind_from = jnp.array(
        [[ring[(places[j] + s) % count] for s in range(count)] for j in range(count)], jnp.int32
    )[me]
    forward = [(ring[k], ring[(k + 1) % count]) for k in range(count)]
    backward = [(ring[(k + 1) % count], ring[k]) for k in range(count)]
    rows = value.shape[0]
    half_rows = rows // 2
    out = jnp.zeros((count,) + value.shape, value.dtype)
    out = lax.dynamic_update_slice(out, value[None], (me, 0, 0))
    ahead, behind = value[:half_rows], value[half_rows:]
    for step in range(1, count):
        ahead = lax.ppermute(ahead, "seq", forward)
        behind = lax.ppermute(behind, "seq", backward)
        source_a = ahead_from[step]
        source_b = behind_from[step]
        out = lax.dynamic_update_slice(out, ahead[None], (source_a, 0, 0))
        out = lax.dynamic_update_slice(out, behind[None], (source_b, half_rows, 0))
    return out.reshape((count * rows,) + value.shape[1:])


def shards(
    ring,
    inputs,
    cotangent,
    pre_attention,
    post_attention,
    pre_feedforward,
    post_feedforward,
    query_weight,
    key_matrix,
    value_matrix,
    output_weight,
    gate_weight,
    up_weight,
    down_weight,
    adapter_down,
    adapter_up,
    prefix_lengths,
    adapter_choice,
):
    groups = lax.axis_size("dp")
    parts = lax.axis_size("mp")
    blocks = lax.axis_size("seq")
    quarters = groups * parts
    own = lax.axis_index("dp")
    part = lax.axis_index("mp")
    quarter = part * groups + own
    rows = inputs.shape[2]
    length = rows * blocks
    positions = lax.axis_index("seq") * rows + jnp.arange(rows, dtype=jnp.int32)
    key_positions = jnp.arange(length, dtype=jnp.int32)
    cosine_table, sine_table = angles(positions)
    query_width = QUERY_HEADS_COUNT * HEAD_SIZE
    key_span_width = KEY_VALUE_HEADS * HEAD_SIZE
    query_local = query_width // quarters
    key_local = key_span_width // quarters
    hidden_local = FF // quarters
    half = MODEL_WIDTH // parts
    head_groups = QUERY_HEADS_COUNT // KEY_VALUE_HEADS
    query_heads = query_local // HEAD_SIZE
    key_heads = key_local // HEAD_SIZE
    row_block = MODEL_WIDTH // (groups * blocks)
    scale = HEAD_SIZE ** (-0.5)
    in_output = 3 * MODEL_WIDTH + quarter * query_local
    in_gate = 3 * MODEL_WIDTH + query_width
    in_up = 4 * MODEL_WIDTH + query_width
    in_down = 5 * MODEL_WIDTH + query_width + quarter * hidden_local
    out_query = quarter * query_local
    out_key = query_width + quarter * key_local
    out_value = query_width + key_span_width + quarter * key_local
    out_output = query_width + 2 * key_span_width
    out_gate = query_width + 2 * key_span_width + MODEL_WIDTH + quarter * hidden_local
    out_up = query_width + 2 * key_span_width + MODEL_WIDTH + FF + quarter * hidden_local
    out_down = query_width + 2 * key_span_width + MODEL_WIDTH + 2 * FF
    tokens = groups * rows
    down_widths = (MODEL_WIDTH, MODEL_WIDTH, MODEL_WIDTH, query_width, MODEL_WIDTH, MODEL_WIDTH, FF)
    up_widths = (query_width, key_span_width, key_span_width, MODEL_WIDTH, FF, FF, MODEL_WIDTH)

    def settle(own_down, own_up, choices_now):
        inner = blocks * parts
        down_chunk = own_down.shape[-1] // (groups * inner)
        up_chunk = own_up.shape[-1] // (groups * inner)
        both = jnp.concatenate(
            [
                own_down.reshape(-1, groups, inner, down_chunk),
                own_up.reshape(-1, groups, inner, up_chunk),
            ],
            axis=-1,
        )
        reduced = lax.psum_scatter(both, ("seq", "mp"), scatter_dimension=2, tiled=True)[:, :, 0]
        reduced = jnp.swapaxes(reduced, 0, 1)
        mine = lax.dynamic_update_index_in_dim(
            jnp.zeros_like(reduced), lax.dynamic_index_in_dim(reduced, own, 0, keepdims=False), own, 0
        )
        for step in range(1, groups):
            send = lax.dynamic_index_in_dim(reduced, wrap(own, step, groups), 0, keepdims=False)
            got = shift(send, "dp", groups, step)
            mine = lax.dynamic_update_index_in_dim(mine, got, wrap(own, -step, groups), 0)
        flat = lax.axis_index(("dp", "seq", "mp"))
        down_part = spread(
            mine[:, :, :down_chunk], choices_now, down_widths, adapter_down.shape[0], flat * down_chunk
        )
        up_part = spread(
            mine[:, :, down_chunk:], choices_now, up_widths, adapter_up.shape[0], flat * up_chunk
        )
        return down_part, up_part

    def to_owner(partial):
        return sum_pairs(scatter_pairs(partial, "dp", groups, own), "mp", parts)

    def permute(value):
        lead = value.shape[:-1]
        moved = value.reshape(lead + (groups, blocks, row_block))
        return jnp.swapaxes(moved, -3, -2).reshape(lead + (MODEL_WIDTH,))

    def unpermute(value):
        lead = value.shape[:-1]
        moved = value.reshape(lead + (blocks, groups, row_block))
        return jnp.swapaxes(moved, -3, -2).reshape(lead + (MODEL_WIDTH,))

    def column_block(weight, index):
        split = weight.reshape(weight.shape[0], groups, -1)
        return lax.dynamic_index_in_dim(split, index, 1, keepdims=False)

    def row_sub(weight, index):
        split = weight.reshape(groups, -1, weight.shape[1])
        return lax.dynamic_index_in_dim(split, index, 0, keepdims=False).T

    column_set = (query_weight, key_matrix, value_matrix)
    row_set = (output_weight,)
    ffw_columns = (gate_weight, up_weight)
    ffw_rows = (down_weight,)

    def swapped(columns, rows_in):
        def block(index):
            return jnp.concatenate(
                [column_block(w, index) for w in columns] + [row_sub(w, index) for w in rows_in], axis=1
            )

        mine = block(own)
        out = lax.dynamic_update_index_in_dim(jnp.zeros((groups,) + mine.shape, mine.dtype), mine, own, 0)
        for step in range(1, groups):
            got = shift(block(wrap(own, step, groups)), "dp", groups, step)
            out = lax.dynamic_update_index_in_dim(out, got, wrap(own, -step, groups), 0)
        return out.reshape(-1, out.shape[-1])

    seq_index = lax.axis_index("seq")
    attention_full = ring_gather(swapped(column_set, row_set), ring, seq_index)
    ffw_full = ring_gather(swapped(ffw_columns, ffw_rows), ring, seq_index)
    cut = [0, query_local, key_local, key_local, query_local]
    edges = np.cumsum(cut).tolist()
    query_full = attention_full[:, edges[0] : edges[1]]
    key_full = attention_full[:, edges[1] : edges[2]]
    value_full = attention_full[:, edges[2] : edges[3]]
    output_full = attention_full[:, edges[3] : edges[4]]
    gate_full = ffw_full[:, :hidden_local]
    up_full = ffw_full[:, hidden_local : 2 * hidden_local]
    down_full = ffw_full[:, 2 * hidden_local :]

    sources_all = jnp.swapaxes(gather_pairs(inputs[:, 0], "dp", groups, own), 0, 1)
    prefix_all = gather_pairs(prefix_lengths[:, 0], "dp", groups, own).T
    choices = jnp.swapaxes(gather_pairs(adapter_choice[:, 0], "dp", groups, own), 0, 1)

    def column_forward(inputs_low, weight, down_part, up_part):
        main = jnp.dot(permute(inputs_low).reshape(tokens, MODEL_WIDTH), weight, preferred_element_type=WIDE)
        inner = jnp.einsum("etd,erd->etr", inputs_low, down_part, preferred_element_type=WIDE).astype(NARROW)
        low = jnp.einsum("etr,ero->eto", inner, up_part, preferred_element_type=WIDE)
        return (main.reshape(groups, rows, -1) + low, inner)

    def row_forward(inputs_low, weight, down_part, up_own):
        width = inputs_low.shape[-1]
        main_part = jnp.einsum(
            "tq,dq->td", inputs_low.reshape(tokens, width), weight, preferred_element_type=WIDE
        )
        inner_part = jnp.einsum("etq,erq->etr", inputs_low, down_part, preferred_element_type=WIDE)
        both = jnp.concatenate([main_part.reshape(groups, rows, MODEL_WIDTH), inner_part], axis=-1)
        both = to_owner(both)
        main = unpermute(both[:, :MODEL_WIDTH])
        inner_low = both[:, MODEL_WIDTH:].astype(NARROW)
        return (main + jnp.dot(inner_low, up_own, preferred_element_type=WIDE), inner_low)

    def column_back(grad_out, weight, down_part, up_part, inputs_low, inner_low):
        inner_grad = jnp.einsum("eto,ero->etr", grad_out, up_part, preferred_element_type=WIDE)
        width = grad_out.shape[-1]
        back = jnp.einsum("to,do->td", grad_out.reshape(tokens, width), weight, preferred_element_type=WIDE)
        back = back.reshape(groups, rows, MODEL_WIDTH)
        back = back + jnp.einsum("etr,erd->etd", inner_grad, permute(down_part).astype(WIDE), precision=HIGH)
        down_grad = jnp.einsum("etr,etd->erd", inner_grad, inputs_low.astype(WIDE), precision=HIGH)
        up_grad = jnp.einsum("etr,eto->ero", inner_low, grad_out, preferred_element_type=WIDE)
        return (back, down_grad, up_grad)

    def row_back(grad_all, grad_own, weight, down_part, up_part, inputs_low, inner_own):
        inner_grad = jnp.einsum("etd,erd->etr", grad_all, up_part, preferred_element_type=WIDE)
        back = jnp.einsum(
            "td,dq->tq", permute(grad_all).reshape(tokens, MODEL_WIDTH), weight, preferred_element_type=WIDE
        )
        back = back.reshape(groups, rows, -1)
        back = back + jnp.einsum("etr,erq->etq", inner_grad, down_part.astype(WIDE), precision=HIGH)
        down_grad = jnp.einsum("etr,etq->erq", inner_grad, inputs_low.astype(WIDE), precision=HIGH)
        own_columns = lax.dynamic_slice_in_dim(grad_own, part * half, half, 1)
        up_grad = jnp.einsum("tr,tc->rc", inner_own, own_columns, preferred_element_type=WIDE)
        return (back, down_grad, up_grad)

    down_list = []
    up_list = []
    results = []
    input_grads = []
    for batch in range(inputs.shape[0]):
        slots = choices[batch]
        own_slots = adapter_choice[batch, 0]
        prefix_length = prefix_all[batch]
        down_query = picks(adapter_down, slots[:, 0], 0, MODEL_WIDTH)
        down_key = picks(adapter_down, slots[:, 1], MODEL_WIDTH, MODEL_WIDTH)
        down_value = picks(adapter_down, slots[:, 2], 2 * MODEL_WIDTH, MODEL_WIDTH)
        down_output = picks(adapter_down, slots[:, 3], in_output, query_local)
        down_gate = picks(adapter_down, slots[:, 4], in_gate, MODEL_WIDTH)
        down_up = picks(adapter_down, slots[:, 5], in_up, MODEL_WIDTH)
        down_down = picks(adapter_down, slots[:, 6], in_down, hidden_local)
        up_query = picks(adapter_up, slots[:, 0], out_query, query_local)
        up_key = picks(adapter_up, slots[:, 1], out_key, key_local)
        up_value = picks(adapter_up, slots[:, 2], out_value, key_local)
        up_output = picks(adapter_up, slots[:, 3], out_output, MODEL_WIDTH)
        up_gate = picks(adapter_up, slots[:, 4], out_gate, hidden_local)
        up_upper = picks(adapter_up, slots[:, 5], out_up, hidden_local)
        up_down = picks(adapter_up, slots[:, 6], out_down, MODEL_WIDTH)
        up_output_own = pick(adapter_up, own_slots[3], out_output, MODEL_WIDTH)
        up_down_own = pick(adapter_up, own_slots[6], out_down, MODEL_WIDTH)

        source = inputs[batch, 0].astype(WIDE)
        normed = normalize(sources_all[batch].astype(WIDE), pre_attention).astype(NARROW)
        query, inner_query = column_forward(normed, query_full, down_query, up_query)
        key_rows, inner_key = column_forward(normed, key_full, down_key, up_key)
        value_rows, inner_value = column_forward(normed, value_full, down_value, up_value)
        rotated_query = apply_rotation(
            query.reshape(groups, rows, query_heads, HEAD_SIZE), cosine_table, sine_table
        ).astype(NARROW)
        rotated_keys = (
            apply_rotation(key_rows.reshape(groups, rows, key_heads, HEAD_SIZE), cosine_table, sine_table)
            .astype(NARROW)
            .reshape(groups, rows, key_local)
        )
        values_low = value_rows.astype(NARROW)
        both_all = lax.all_gather(jnp.stack([rotated_keys, values_low]), "seq", axis=2, tiled=True)
        keys_three = both_all[0].reshape(groups, length, key_heads, HEAD_SIZE)
        values_three = both_all[1].reshape(groups, length, key_heads, HEAD_SIZE)
        query_four = rotated_query.reshape(groups, rows, key_heads, head_groups, HEAD_SIZE)
        visible = (key_positions[None, None, :] <= positions[None, :, None]) | (
            key_positions[None, None, :] < prefix_length[:, None, None]
        )
        visible = visible[:, None, None]
        raw = (
            jnp.einsum("etkgd,eskd->ekgts", query_four, keys_three, preferred_element_type=WIDE)
            * scale
        )
        masked = jnp.where(visible, SOFT_CAP * jnp.tanh(raw / SOFT_CAP), -1e30)
        top = jnp.max(masked, axis=-1, keepdims=True)
        expo = jnp.exp(masked - top)
        total = jnp.sum(expo, axis=-1, keepdims=True)
        log_total = top + jnp.log(total)
        prob_low = (expo / total).astype(NARROW)
        head_stack = jnp.einsum(
            "ekgts,eskd->etkgd", prob_low, values_three, preferred_element_type=WIDE
        )
        head_stack = head_stack.reshape(groups, rows, query_local).astype(NARROW)
        attention_out, inner_output = row_forward(head_stack, output_full, down_output, up_output_own)
        middle = source + normalize(attention_out, post_attention)
        normed_ffw_own = normalize(middle, pre_feedforward).astype(NARROW)
        normed_ffw = gather_pairs(normed_ffw_own, "dp", groups, own)
        gate, inner_gate = column_forward(normed_ffw, gate_full, down_gate, up_gate)
        upper, inner_upper = column_forward(normed_ffw, up_full, down_up, up_upper)
        hidden = activate(gate, upper).astype(NARROW)
        ffw_out, inner_down = row_forward(hidden, down_full, down_down, up_down_own)
        results.append((middle + normalize(ffw_out, post_feedforward)).astype(NARROW))

        grad_down = jnp.zeros((groups,) + adapter_down.shape[1:], WIDE)
        grad_up = jnp.zeros((groups,) + adapter_up.shape[1:], WIDE)
        seed_grad = cotangent[batch, 0].astype(WIDE)
        grad_ffw_own = normalize_back(ffw_out, post_feedforward, seed_grad).astype(NARROW)
        grad_ffw = gather_pairs(grad_ffw_own, "dp", groups, own)
        grad_hidden, piece_down, piece_up = row_back(
            grad_ffw, grad_ffw_own, down_full, down_down, up_down, hidden, inner_down
        )
        grad_down = place(grad_down, piece_down, in_down)
        grad_up = place_own(grad_up, piece_up, own, out_down + part * half)
        pull = jax.vjp(activate, gate, upper)[1]
        grad_gate, grad_upper = pull(grad_hidden)
        grad_gate = grad_gate.astype(NARROW)
        grad_upper = grad_upper.astype(NARROW)
        back_gate, piece_down, piece_up = column_back(
            grad_gate, gate_full, down_gate, up_gate, normed_ffw, inner_gate
        )
        grad_down = place(grad_down, piece_down, in_gate)
        grad_up = place(grad_up, piece_up, out_gate)
        back_upper, piece_down, piece_up = column_back(
            grad_upper, up_full, down_up, up_upper, normed_ffw, inner_upper
        )
        grad_down = place(grad_down, piece_down, in_up)
        grad_up = place(grad_up, piece_up, out_up)
        grad_normed_ffw = unpermute(to_owner(back_gate + back_upper))
        grad_middle = seed_grad + normalize_back(middle, pre_feedforward, grad_normed_ffw)
        grad_attention_own = normalize_back(attention_out, post_attention, grad_middle).astype(NARROW)
        grad_attention = gather_pairs(grad_attention_own, "dp", groups, own)
        grad_heads, piece_down, piece_up = row_back(
            grad_attention,
            grad_attention_own,
            output_full,
            down_output,
            up_output,
            head_stack,
            inner_output,
        )
        grad_down = place(grad_down, piece_down, in_output)
        grad_up = place_own(grad_up, piece_up, own, out_output + part * half)
        grad_heads_four = grad_heads.astype(NARROW).reshape(groups, rows, key_heads, head_groups, HEAD_SIZE)
        prob = jnp.exp(masked - log_total)
        grad_prob = jnp.einsum(
            "etkgd,eskd->ekgts", grad_heads_four, values_three, preferred_element_type=WIDE
        )
        grad_capped = prob * (grad_prob - jnp.sum(prob * grad_prob, axis=-1, keepdims=True))
        bend = jnp.tanh(raw / SOFT_CAP)
        grad_raw = (grad_capped * (1.0 - bend * bend)).astype(NARROW)
        grad_query_rot = (
            jnp.einsum("ekgts,eskd->etkgd", grad_raw, keys_three, preferred_element_type=WIDE) * scale
        )
        grad_key_part = (
            jnp.einsum("ekgts,etkgd->eskd", grad_raw, query_four, preferred_element_type=WIDE) * scale
        )
        grad_value_part = jnp.einsum(
            "ekgts,etkgd->eskd", prob_low, grad_heads_four, preferred_element_type=WIDE
        )
        both_grad = lax.psum_scatter(
            jnp.stack(
                [
                    grad_key_part.reshape(groups, length, key_local),
                    grad_value_part.reshape(groups, length, key_local),
                ]
            ),
            "seq",
            scatter_dimension=2,
            tiled=True,
        )
        key_grad, value_grad = both_grad[0], both_grad[1]
        grad_query = (
            rotate_back(
                grad_query_rot.reshape(groups, rows, query_heads, HEAD_SIZE), cosine_table, sine_table
            )
            .reshape(groups, rows, query_local)
            .astype(NARROW)
        )
        grad_key = (
            rotate_back(key_grad.reshape(groups, rows, key_heads, HEAD_SIZE), cosine_table, sine_table)
            .reshape(groups, rows, key_local)
            .astype(NARROW)
        )
        grad_value = value_grad.astype(NARROW)
        back_query, piece_down, piece_up = column_back(
            grad_query, query_full, down_query, up_query, normed, inner_query
        )
        grad_down = place(grad_down, piece_down, 0)
        grad_up = place(grad_up, piece_up, out_query)
        back_key, piece_down, piece_up = column_back(
            grad_key, key_full, down_key, up_key, normed, inner_key
        )
        grad_down = place(grad_down, piece_down, MODEL_WIDTH)
        grad_up = place(grad_up, piece_up, out_key)
        back_value, piece_down, piece_up = column_back(
            grad_value, value_full, down_value, up_value, normed, inner_value
        )
        grad_down = place(grad_down, piece_down, 2 * MODEL_WIDTH)
        grad_up = place(grad_up, piece_up, out_value)
        grad_normed = unpermute(to_owner(back_query + back_key + back_value))
        own_down = scatter_pairs(grad_down, "dp", groups, own)
        own_up = scatter_pairs(grad_up, "dp", groups, own)
        down_part, up_part = settle(own_down, own_up, slots)
        down_list.append(down_part)
        up_list.append(up_part)
        input_grads.append(
            (grad_middle + normalize_back(source, pre_attention, grad_normed)).astype(NARROW)
        )
    down_total = down_list[0]
    up_total = up_list[0]
    for extra in range(1, len(down_list)):
        down_total = down_total + down_list[extra]
        up_total = up_total + up_list[extra]
    outputs = jnp.stack(results)[:, None]
    input_gradient = jnp.stack(input_grads)[:, None]
    return (outputs, input_gradient, down_total, up_total)


def solution(mesh):
    ring = ring_order(mesh)

    def body(*args):
        return shards(ring, *args)

    return jax.shard_map(
        body,
        mesh=mesh,
        in_specs=(
            P(None, "dp", "seq", None),
            P(None, "dp", "seq", None),
            P(),
            P(),
            P(),
            P(),
            P(("dp", "seq"), "mp"),
            P(("dp", "seq"), "mp"),
            P(("dp", "seq"), "mp"),
            P("mp", ("dp", "seq")),
            P(("dp", "seq"), "mp"),
            P(("dp", "seq"), "mp"),
            P("mp", ("dp", "seq")),
            P(),
            P(),
            P(None, "dp"),
            P(None, "dp", None),
        ),
        out_specs=(
            P(None, "dp", "seq", None),
            P(None, "dp", "seq", None),
            P(None, None, ("dp", "seq", "mp")),
            P(None, None, ("dp", "seq", "mp")),
        ),
        check_vma=False,
    )
```

```python
import numpy as np
import jax
import jax.numpy as jnp
from jax import lax
from jax.sharding import PartitionSpec as P

MODEL_WIDTH = 2304
QUERY_HEADS_COUNT = 8
KEY_VALUE_HEADS = 4
HEAD_SIZE = 256
FF = 9216


HIGH = lax.Precision.HIGHEST
EPSILON = 1e-06
SOFT_CAP = 50.0
WIDE = jnp.float32
NARROW = jnp.bfloat16


def normalize(value, gain):
    factor = lax.rsqrt(jnp.mean(value * value, axis=-1, keepdims=True) + EPSILON)
    return value * factor * gain


def normalize_back(value, gain, upstream):
    factor = lax.rsqrt(jnp.mean(value * value, axis=-1, keepdims=True) + EPSILON)
    scaled = upstream * gain
    inner = jnp.mean(value * scaled, axis=-1, keepdims=True)
    return factor * scaled - value * (factor * factor * factor) * inner


def angles(positions):
    half = HEAD_SIZE // 2
    rates = 10000.0 ** (-(jnp.arange(half, dtype=WIDE) * 2.0) / HEAD_SIZE)
    turns = positions.astype(WIDE)[:, None] * rates[None, :]
    return (jnp.cos(turns)[:, None, :], jnp.sin(turns)[:, None, :])


def apply_rotation(head_stack, cosine_table, sine_table):
    half = HEAD_SIZE // 2
    first = head_stack[..., :half]
    second = head_stack[..., half:]
    return jnp.concatenate(
        [first * cosine_table - second * sine_table, second * cosine_table + first * sine_table],
        axis=-1,
    )


def rotate_back(grads, cosine_table, sine_table):
    half = HEAD_SIZE // 2
    first = grads[..., :half]
    second = grads[..., half:]
    return jnp.concatenate(
        [first * cosine_table + second * sine_table, second * cosine_table - first * sine_table],
        axis=-1,
    )


def pick(table, index, start_index, size):
    window = lax.dynamic_slice_in_dim(table, start_index, size, axis=2)
    hit = jnp.arange(table.shape[0], dtype=jnp.int32) == index
    return jnp.sum(jnp.where(hit[:, None, None], window.astype(WIDE), 0.0), axis=0).astype(table.dtype)


def picks(table, slots, start_index, size):
    return jnp.stack([pick(table, slots[e], start_index, size) for e in range(slots.shape[0])])


def place(total, piece, start_index):
    return lax.dynamic_update_slice(total, piece, (0, 0, start_index))


def place_own(total, piece, own, start_index):
    return lax.dynamic_update_slice(total, piece[None], (own, 0, start_index))


def activate(gate_value, up_value):
    return jax.nn.gelu(gate_value, approximate=True) * up_value


def segment_of(columns, widths):
    seg = jnp.zeros(columns.shape, jnp.int32)
    edge = 0
    for width in widths[:-1]:
        edge += width
        seg = seg + (columns >= edge).astype(jnp.int32)
    return seg


def spread(compact, choices, widths, adapters, start):
    columns = start + jnp.arange(compact.shape[-1], dtype=jnp.int32)
    seg = segment_of(columns, widths)
    chosen = jnp.zeros((choices.shape[0], compact.shape[-1]), jnp.int32)
    for index in range(len(widths)):
        chosen = chosen + jnp.where(seg == index, choices[:, index : index + 1], 0)
    hits = chosen[None] == jnp.arange(adapters, dtype=jnp.int32)[:, None, None]
    picked = jnp.where(hits[:, :, None, :], compact[None], 0.0)
    return jnp.sum(picked, axis=1)


def snake(sizes):
    if not sizes:
        return [()]
    inner = snake(sizes[1:])
    order = []
    for value in range(sizes[0]):
        steps = inner if value % 2 == 0 else inner[::-1]
        order.extend((value,) + rest for rest in steps)
    return order


def ring_order(mesh):
    names = tuple(mesh.axis_names)
    count = mesh.shape["seq"]
    where = [0] * len(names)
    members = []
    for index in range(count):
        where[names.index("seq")] = index
        members.append(mesh.devices[tuple(where)])
    try:
        coords = np.array([list(dev.coords) + [int(getattr(dev, "core_on_chip", 0))] for dev in members])
    except Exception:
        return list(range(count))
    varying = [k for k in range(coords.shape[1]) if len(set(coords[:, k].tolist())) > 1]
    sizes = [len(set(coords[:, k].tolist())) for k in varying]
    if int(np.prod(sizes)) != count:
        return list(range(count))
    lowest = coords[:, varying].min(axis=0)
    lookup = {tuple((coords[i, varying] - lowest).tolist()): i for i in range(count)}
    if len(lookup) != count:
        return list(range(count))
    pairs = [k for k in range(len(sizes)) if sizes[k] == 2]
    if pairs:
        pivot = pairs[-1]
        rest = [sizes[k] for k in range(len(sizes)) if k != pivot]
        path = snake(rest)
        order = []
        for value, steps in ((0, path), (1, path[::-1])):
            for point in steps:
                full = list(point)
                full.insert(pivot, value)
                order.append(full)
    else:
        order = [list(point) for point in snake(sizes)]
    return [lookup[tuple(point)] for point in order]


def wrap(index, step, size):
    return jnp.array([(a + step) % size for a in range(size)], jnp.int32)[index]


def shift(value, axis, size, step):
    return lax.ppermute(value, axis, [(a, (a + step) % size) for a in range(size)])


def gather_pairs(value, axis, size, me):
    out = jnp.zeros((size,) + value.shape, value.dtype)
    out = lax.dynamic_update_index_in_dim(out, value, me, 0)
    for step in range(1, size):
        got = shift(value, axis, size, step)
        out = lax.dynamic_update_index_in_dim(out, got, wrap(me, -step, size), 0)
    return out


def scatter_pairs(partial, axis, size, me):
    mine = lax.dynamic_index_in_dim(partial, me, 0, keepdims=False)
    for step in range(1, size):
        send = lax.dynamic_index_in_dim(partial, wrap(me, step, size), 0, keepdims=False)
        mine = mine + shift(send, axis, size, step)
    return mine


def sum_pairs(value, axis, size):
    total = value
    for step in range(1, size):
        total = total + shift(value, axis, size, step)
    return total


def ring_gather(value, ring, me):
    count = len(ring)
    places = [0] * count
    for k, member in enumerate(ring):
        places[member] = k
    ahead_from = jnp.array(
        [[ring[(places[j] - s) % count] for s in range(count)] for j in range(count)], jnp.int32
    )[me]
    behind_from = jnp.array(
        [[ring[(places[j] + s) % count] for s in range(count)] for j in range(count)], jnp.int32
    )[me]
    forward = [(ring[k], ring[(k + 1) % count]) for k in range(count)]
    backward = [(ring[(k + 1) % count], ring[k]) for k in range(count)]
    rows = value.shape[0]
    half_rows = rows // 2
    out = jnp.zeros((count,) + value.shape, value.dtype)
    out = lax.dynamic_update_slice(out, value[None], (me, 0, 0))
    ahead, behind = value[:half_rows], value[half_rows:]
    for step in range(1, count):
        ahead = lax.ppermute(ahead, "seq", forward)
        behind = lax.ppermute(behind, "seq", backward)
        source_a = ahead_from[step]
        source_b = behind_from[step]
        out = lax.dynamic_update_slice(out, ahead[None], (source_a, 0, 0))
        out = lax.dynamic_update_slice(out, behind[None], (source_b, half_rows, 0))
    return out.reshape((count * rows,) + value.shape[1:])


def shards(
    ring,
    inputs,
    cotangent,
    pre_attention,
    post_attention,
    pre_feedforward,
    post_feedforward,
    query_weight,
    key_matrix,
    value_matrix,
    output_weight,
    gate_weight,
    up_weight,
    down_weight,
    adapter_down,
    adapter_up,
    prefix_lengths,
    adapter_choice,
):
    groups = lax.axis_size("dp")
    parts = lax.axis_size("mp")
    blocks = lax.axis_size("seq")
    quarters = groups * parts
    own = lax.axis_index("dp")
    part = lax.axis_index("mp")
    quarter = part * groups + own
    rows = inputs.shape[2]
    length = rows * blocks
    positions = lax.axis_index("seq") * rows + jnp.arange(rows, dtype=jnp.int32)
    key_positions = jnp.arange(length, dtype=jnp.int32)
    cosine_table, sine_table = angles(positions)
    query_width = QUERY_HEADS_COUNT * HEAD_SIZE
    key_span_width = KEY_VALUE_HEADS * HEAD_SIZE
    query_local = query_width // quarters
    key_local = key_span_width // quarters
    hidden_local = FF // quarters
    half = MODEL_WIDTH // parts
    head_groups = QUERY_HEADS_COUNT // KEY_VALUE_HEADS
    query_heads = query_local // HEAD_SIZE
    key_heads = key_local // HEAD_SIZE
    row_block = MODEL_WIDTH // (groups * blocks)
    scale = HEAD_SIZE ** (-0.5)
    in_output = 3 * MODEL_WIDTH + quarter * query_local
    in_gate = 3 * MODEL_WIDTH + query_width
    in_up = 4 * MODEL_WIDTH + query_width
    in_down = 5 * MODEL_WIDTH + query_width + quarter * hidden_local
    out_query = quarter * query_local
    out_key = query_width + quarter * key_local
    out_value = query_width + key_span_width + quarter * key_local
    out_output = query_width + 2 * key_span_width
    out_gate = query_width + 2 * key_span_width + MODEL_WIDTH + quarter * hidden_local
    out_up = query_width + 2 * key_span_width + MODEL_WIDTH + FF + quarter * hidden_local
    out_down = query_width + 2 * key_span_width + MODEL_WIDTH + 2 * FF
    tokens = groups * rows
    down_widths = (MODEL_WIDTH, MODEL_WIDTH, MODEL_WIDTH, query_width, MODEL_WIDTH, MODEL_WIDTH, FF)
    up_widths = (query_width, key_span_width, key_span_width, MODEL_WIDTH, FF, FF, MODEL_WIDTH)

    def settle(own_down, own_up, choices_now):
        inner = blocks * parts
        down_chunk = own_down.shape[-1] // (groups * inner)
        up_chunk = own_up.shape[-1] // (groups * inner)
        both = jnp.concatenate(
            [
                own_down.reshape(-1, groups, inner, down_chunk),
                own_up.reshape(-1, groups, inner, up_chunk),
            ],
            axis=-1,
        )
        reduced = lax.psum_scatter(both, ("seq", "mp"), scatter_dimension=2, tiled=True)[:, :, 0]
        reduced = jnp.swapaxes(reduced, 0, 1)
        mine = lax.dynamic_update_index_in_dim(
            jnp.zeros_like(reduced), lax.dynamic_index_in_dim(reduced, own, 0, keepdims=False), own, 0
        )
        for step in range(1, groups):
            send = lax.dynamic_index_in_dim(reduced, wrap(own, step, groups), 0, keepdims=False)
            got = shift(send, "dp", groups, step)
            mine = lax.dynamic_update_index_in_dim(mine, got, wrap(own, -step, groups), 0)
        flat = lax.axis_index(("dp", "seq", "mp"))
        down_part = spread(
            mine[:, :, :down_chunk], choices_now, down_widths, adapter_down.shape[0], flat * down_chunk
        )
        up_part = spread(
            mine[:, :, down_chunk:], choices_now, up_widths, adapter_up.shape[0], flat * up_chunk
        )
        return down_part, up_part

    def exchange_adapters(grad_down, grad_up):
        if groups != 2:
            return scatter_pairs(grad_down, "dp", groups, own), scatter_pairs(grad_up, "dp", groups, own)
        other = wrap(own, 1, groups)
        sender = part * groups + other

        def spans(which):
            if which == "down":
                return [
                    (0, 3 * MODEL_WIDTH),
                    (in_gate, 2 * MODEL_WIDTH),
                    (3 * MODEL_WIDTH + which_quarter * query_local, query_local),
                    (5 * MODEL_WIDTH + query_width + which_quarter * hidden_local, hidden_local),
                ]
            return [
                (which_quarter * query_local, query_local),
                (query_width + which_quarter * key_local, key_local),
                (query_width + key_span_width + which_quarter * key_local, key_local),
                (query_width + 2 * key_span_width + MODEL_WIDTH + which_quarter * hidden_local, hidden_local),
                (query_width + 2 * key_span_width + MODEL_WIDTH + FF + which_quarter * hidden_local, hidden_local),
            ]

        results = []
        for which, table in (("down", grad_down), ("up", grad_up)):
            which_quarter = quarter
            send = lax.dynamic_index_in_dim(table, other, 0, keepdims=False)
            packed = jnp.concatenate(
                [lax.dynamic_slice_in_dim(send, start, size, axis=1) for start, size in spans(which)], axis=1
            )
            got = shift(packed, "dp", groups, 1)
            which_quarter = sender
            total = lax.dynamic_index_in_dim(table, own, 0, keepdims=False)
            landed = jnp.zeros_like(total)
            offset = 0
            for start, size in spans(which):
                landed = lax.dynamic_update_slice_in_dim(landed, got[:, offset : offset + size], start, axis=1)
                offset += size
            results.append(total + landed)
        return results[0], results[1]

    def to_owner(partial):
        return sum_pairs(scatter_pairs(partial, "dp", groups, own), "mp", parts)

    def permute(value):
        lead = value.shape[:-1]
        moved = value.reshape(lead + (groups, blocks, row_block))
        return jnp.swapaxes(moved, -3, -2).reshape(lead + (MODEL_WIDTH,))

    def unpermute(value):
        lead = value.shape[:-1]
        moved = value.reshape(lead + (blocks, groups, row_block))
        return jnp.swapaxes(moved, -3, -2).reshape(lead + (MODEL_WIDTH,))

    def column_block(weight, index):
        split = weight.reshape(weight.shape[0], groups, -1)
        return lax.dynamic_index_in_dim(split, index, 1, keepdims=False)

    def row_sub(weight, index):
        split = weight.reshape(groups, -1, weight.shape[1])
        return lax.dynamic_index_in_dim(split, index, 0, keepdims=False).T

    column_set = (query_weight, key_matrix, value_matrix)
    row_set = (output_weight,)
    ffw_columns = (gate_weight, up_weight)
    ffw_rows = (down_weight,)

    def swapped(columns, rows_in):
        def block(index):
            return jnp.concatenate(
                [column_block(w, index) for w in columns] + [row_sub(w, index) for w in rows_in], axis=1
            )

        mine = block(own)
        out = lax.dynamic_update_index_in_dim(jnp.zeros((groups,) + mine.shape, mine.dtype), mine, own, 0)
        for step in range(1, groups):
            got = shift(block(wrap(own, step, groups)), "dp", groups, step)
            out = lax.dynamic_update_index_in_dim(out, got, wrap(own, -step, groups), 0)
        return out.reshape(-1, out.shape[-1])

    seq_index = lax.axis_index("seq")
    attention_full = ring_gather(swapped(column_set, row_set), ring, seq_index)
    ffw_full = ring_gather(swapped(ffw_columns, ffw_rows), ring, seq_index)
    cut = [0, query_local, key_local, key_local, query_local]
    edges = np.cumsum(cut).tolist()
    query_full = attention_full[:, edges[0] : edges[1]]
    key_full = attention_full[:, edges[1] : edges[2]]
    value_full = attention_full[:, edges[2] : edges[3]]
    output_full = attention_full[:, edges[3] : edges[4]]
    gate_full = ffw_full[:, :hidden_local]
    up_full = ffw_full[:, hidden_local : 2 * hidden_local]
    down_full = ffw_full[:, 2 * hidden_local :]

    sources_all = jnp.swapaxes(gather_pairs(inputs[:, 0], "dp", groups, own), 0, 1)
    prefix_all = gather_pairs(prefix_lengths[:, 0], "dp", groups, own).T
    choices = jnp.swapaxes(gather_pairs(adapter_choice[:, 0], "dp", groups, own), 0, 1)

    def column_forward(inputs_low, weight, down_part, up_part):
        main = jnp.dot(permute(inputs_low).reshape(tokens, MODEL_WIDTH), weight, preferred_element_type=WIDE)
        inner = jnp.einsum("etd,erd->etr", inputs_low, down_part, preferred_element_type=WIDE).astype(NARROW)
        low = jnp.einsum("etr,ero->eto", inner, up_part, preferred_element_type=WIDE)
        return (main.reshape(groups, rows, -1) + low, inner)

    def row_forward(inputs_low, weight, down_part, up_own):
        width = inputs_low.shape[-1]
        main_part = jnp.einsum(
            "tq,dq->td", inputs_low.reshape(tokens, width), weight, preferred_element_type=WIDE
        )
        inner_part = jnp.einsum("etq,erq->etr", inputs_low, down_part, preferred_element_type=WIDE)
        both = jnp.concatenate([main_part.reshape(groups, rows, MODEL_WIDTH), inner_part], axis=-1)
        both = to_owner(both)
        main = unpermute(both[:, :MODEL_WIDTH])
        inner_low = both[:, MODEL_WIDTH:].astype(NARROW)
        return (main + jnp.dot(inner_low, up_own, preferred_element_type=WIDE), inner_low)

    def column_back(grad_out, weight, down_part, up_part, inputs_low, inner_low):
        inner_grad = jnp.einsum("eto,ero->etr", grad_out, up_part, preferred_element_type=WIDE)
        width = grad_out.shape[-1]
        back = jnp.einsum("to,do->td", grad_out.reshape(tokens, width), weight, preferred_element_type=WIDE)
        back = back.reshape(groups, rows, MODEL_WIDTH)
        back = back + jnp.einsum("etr,erd->etd", inner_grad, permute(down_part).astype(WIDE), precision=HIGH)
        down_grad = jnp.einsum("etr,etd->erd", inner_grad, inputs_low.astype(WIDE), precision=HIGH)
        up_grad = jnp.einsum("etr,eto->ero", inner_low, grad_out, preferred_element_type=WIDE)
        return (back, down_grad, up_grad)

    def row_back(grad_all, grad_own, weight, down_part, up_part, inputs_low, inner_own):
        inner_grad = jnp.einsum("etd,erd->etr", grad_all, up_part, preferred_element_type=WIDE)
        back = jnp.einsum(
            "td,dq->tq", permute(grad_all).reshape(tokens, MODEL_WIDTH), weight, preferred_element_type=WIDE
        )
        back = back.reshape(groups, rows, -1)
        back = back + jnp.einsum("etr,erq->etq", inner_grad, down_part.astype(WIDE), precision=HIGH)
        down_grad = jnp.einsum("etr,etq->erq", inner_grad, inputs_low.astype(WIDE), precision=HIGH)
        own_columns = lax.dynamic_slice_in_dim(grad_own, part * half, half, 1)
        up_grad = jnp.einsum("tr,tc->rc", inner_own, own_columns, preferred_element_type=WIDE)
        return (back, down_grad, up_grad)

    down_list = []
    up_list = []
    results = []
    input_grads = []
    for batch in range(inputs.shape[0]):
        slots = choices[batch]
        own_slots = adapter_choice[batch, 0]
        prefix_length = prefix_all[batch]
        down_query = picks(adapter_down, slots[:, 0], 0, MODEL_WIDTH)
        down_key = picks(adapter_down, slots[:, 1], MODEL_WIDTH, MODEL_WIDTH)
        down_value = picks(adapter_down, slots[:, 2], 2 * MODEL_WIDTH, MODEL_WIDTH)
        down_output = picks(adapter_down, slots[:, 3], in_output, query_local)
        down_gate = picks(adapter_down, slots[:, 4], in_gate, MODEL_WIDTH)
        down_up = picks(adapter_down, slots[:, 5], in_up, MODEL_WIDTH)
        down_down = picks(adapter_down, slots[:, 6], in_down, hidden_local)
        up_query = picks(adapter_up, slots[:, 0], out_query, query_local)
        up_key = picks(adapter_up, slots[:, 1], out_key, key_local)
        up_value = picks(adapter_up, slots[:, 2], out_value, key_local)
        up_output = picks(adapter_up, slots[:, 3], out_output, MODEL_WIDTH)
        up_gate = picks(adapter_up, slots[:, 4], out_gate, hidden_local)
        up_upper = picks(adapter_up, slots[:, 5], out_up, hidden_local)
        up_down = picks(adapter_up, slots[:, 6], out_down, MODEL_WIDTH)
        up_output_own = pick(adapter_up, own_slots[3], out_output, MODEL_WIDTH)
        up_down_own = pick(adapter_up, own_slots[6], out_down, MODEL_WIDTH)

        source = inputs[batch, 0].astype(WIDE)
        normed = normalize(sources_all[batch].astype(WIDE), pre_attention).astype(NARROW)
        query, inner_query = column_forward(normed, query_full, down_query, up_query)
        key_rows, inner_key = column_forward(normed, key_full, down_key, up_key)
        value_rows, inner_value = column_forward(normed, value_full, down_value, up_value)
        rotated_query = apply_rotation(
            query.reshape(groups, rows, query_heads, HEAD_SIZE), cosine_table, sine_table
        ).astype(NARROW)
        rotated_keys = (
            apply_rotation(key_rows.reshape(groups, rows, key_heads, HEAD_SIZE), cosine_table, sine_table)
            .astype(NARROW)
            .reshape(groups, rows, key_local)
        )
        values_low = value_rows.astype(NARROW)
        both_all = lax.all_gather(jnp.stack([rotated_keys, values_low]), "seq", axis=2, tiled=True)
        keys_three = both_all[0].reshape(groups, length, key_heads, HEAD_SIZE)
        values_three = both_all[1].reshape(groups, length, key_heads, HEAD_SIZE)
        query_four = rotated_query.reshape(groups, rows, key_heads, head_groups, HEAD_SIZE)
        visible = (key_positions[None, None, :] <= positions[None, :, None]) | (
            key_positions[None, None, :] < prefix_length[:, None, None]
        )
        visible = visible[:, None, None]
        raw = (
            jnp.einsum("etkgd,eskd->ekgts", query_four, keys_three, preferred_element_type=WIDE)
            * scale
        )
        masked = jnp.where(visible, SOFT_CAP * jnp.tanh(raw / SOFT_CAP), -1e30)
        top = jnp.max(masked, axis=-1, keepdims=True)
        expo = jnp.exp(masked - top)
        total = jnp.sum(expo, axis=-1, keepdims=True)
        log_total = top + jnp.log(total)
        prob_low = (expo / total).astype(NARROW)
        head_stack = jnp.einsum(
            "ekgts,eskd->etkgd", prob_low, values_three, preferred_element_type=WIDE
        )
        head_stack = head_stack.reshape(groups, rows, query_local).astype(NARROW)
        attention_out, inner_output = row_forward(head_stack, output_full, down_output, up_output_own)
        middle = source + normalize(attention_out, post_attention)
        normed_ffw_own = normalize(middle, pre_feedforward).astype(NARROW)
        normed_ffw = gather_pairs(normed_ffw_own, "dp", groups, own)
        gate, inner_gate = column_forward(normed_ffw, gate_full, down_gate, up_gate)
        upper, inner_upper = column_forward(normed_ffw, up_full, down_up, up_upper)
        hidden = activate(gate, upper).astype(NARROW)
        ffw_out, inner_down = row_forward(hidden, down_full, down_down, up_down_own)
        results.append((middle + normalize(ffw_out, post_feedforward)).astype(NARROW))

        grad_down = jnp.zeros((groups,) + adapter_down.shape[1:], WIDE)
        grad_up = jnp.zeros((groups,) + adapter_up.shape[1:], WIDE)
        seed_grad = cotangent[batch, 0].astype(WIDE)
        grad_ffw_own = normalize_back(ffw_out, post_feedforward, seed_grad).astype(NARROW)
        grad_ffw = gather_pairs(grad_ffw_own, "dp", groups, own)
        grad_hidden, piece_down, piece_up = row_back(
            grad_ffw, grad_ffw_own, down_full, down_down, up_down, hidden, inner_down
        )
        grad_down = place(grad_down, piece_down, in_down)
        grad_up = place_own(grad_up, piece_up, own, out_down + part * half)
        pull = jax.vjp(activate, gate, upper)[1]
        grad_gate, grad_upper = pull(grad_hidden)
        grad_gate = grad_gate.astype(NARROW)
        grad_upper = grad_upper.astype(NARROW)
        back_gate, piece_down, piece_up = column_back(
            grad_gate, gate_full, down_gate, up_gate, normed_ffw, inner_gate
        )
        grad_down = place(grad_down, piece_down, in_gate)
        grad_up = place(grad_up, piece_up, out_gate)
        back_upper, piece_down, piece_up = column_back(
            grad_upper, up_full, down_up, up_upper, normed_ffw, inner_upper
        )
        grad_down = place(grad_down, piece_down, in_up)
        grad_up = place(grad_up, piece_up, out_up)
        grad_normed_ffw = unpermute(to_owner(back_gate + back_upper))
        grad_middle = seed_grad + normalize_back(middle, pre_feedforward, grad_normed_ffw)
        grad_attention_own = normalize_back(attention_out, post_attention, grad_middle).astype(NARROW)
        grad_attention = gather_pairs(grad_attention_own, "dp", groups, own)
        grad_heads, piece_down, piece_up = row_back(
            grad_attention,
            grad_attention_own,
            output_full,
            down_output,
            up_output,
            head_stack,
            inner_output,
        )
        grad_down = place(grad_down, piece_down, in_output)
        grad_up = place_own(grad_up, piece_up, own, out_output + part * half)
        grad_heads_four = grad_heads.astype(NARROW).reshape(groups, rows, key_heads, head_groups, HEAD_SIZE)
        prob = jnp.exp(masked - log_total)
        grad_prob = jnp.einsum(
            "etkgd,eskd->ekgts", grad_heads_four, values_three, preferred_element_type=WIDE
        )
        grad_capped = prob * (grad_prob - jnp.sum(prob * grad_prob, axis=-1, keepdims=True))
        bend = jnp.tanh(raw / SOFT_CAP)
        grad_raw = (grad_capped * (1.0 - bend * bend)).astype(NARROW)
        grad_query_rot = (
            jnp.einsum("ekgts,eskd->etkgd", grad_raw, keys_three, preferred_element_type=WIDE) * scale
        )
        grad_key_part = (
            jnp.einsum("ekgts,etkgd->eskd", grad_raw, query_four, preferred_element_type=WIDE) * scale
        )
        grad_value_part = jnp.einsum(
            "ekgts,etkgd->eskd", prob_low, grad_heads_four, preferred_element_type=WIDE
        )
        both_grad = lax.psum_scatter(
            jnp.stack(
                [
                    grad_key_part.reshape(groups, length, key_local),
                    grad_value_part.reshape(groups, length, key_local),
                ]
            ),
            "seq",
            scatter_dimension=2,
            tiled=True,
        )
        key_grad, value_grad = both_grad[0], both_grad[1]
        grad_query = (
            rotate_back(
                grad_query_rot.reshape(groups, rows, query_heads, HEAD_SIZE), cosine_table, sine_table
            )
            .reshape(groups, rows, query_local)
            .astype(NARROW)
        )
        grad_key = (
            rotate_back(key_grad.reshape(groups, rows, key_heads, HEAD_SIZE), cosine_table, sine_table)
            .reshape(groups, rows, key_local)
            .astype(NARROW)
        )
        grad_value = value_grad.astype(NARROW)
        back_query, piece_down, piece_up = column_back(
            grad_query, query_full, down_query, up_query, normed, inner_query
        )
        grad_down = place(grad_down, piece_down, 0)
        grad_up = place(grad_up, piece_up, out_query)
        back_key, piece_down, piece_up = column_back(
            grad_key, key_full, down_key, up_key, normed, inner_key
        )
        grad_down = place(grad_down, piece_down, MODEL_WIDTH)
        grad_up = place(grad_up, piece_up, out_key)
        back_value, piece_down, piece_up = column_back(
            grad_value, value_full, down_value, up_value, normed, inner_value
        )
        grad_down = place(grad_down, piece_down, 2 * MODEL_WIDTH)
        grad_up = place(grad_up, piece_up, out_value)
        grad_normed = unpermute(to_owner(back_query + back_key + back_value))
        own_down, own_up = exchange_adapters(grad_down, grad_up)
        down_part, up_part = settle(own_down, own_up, slots)
        down_list.append(down_part)
        up_list.append(up_part)
        input_grads.append(
            (grad_middle + normalize_back(source, pre_attention, grad_normed)).astype(NARROW)
        )
    down_total = down_list[0]
    up_total = up_list[0]
    for extra in range(1, len(down_list)):
        down_total = down_total + down_list[extra]
        up_total = up_total + up_list[extra]
    outputs = jnp.stack(results)[:, None]
    input_gradient = jnp.stack(input_grads)[:, None]
    return (outputs, input_gradient, down_total, up_total)


def solution(mesh):
    ring = ring_order(mesh)

    def body(*args):
        return shards(ring, *args)

    return jax.shard_map(
        body,
        mesh=mesh,
        in_specs=(
            P(None, "dp", "seq", None),
            P(None, "dp", "seq", None),
            P(),
            P(),
            P(),
            P(),
            P(("dp", "seq"), "mp"),
            P(("dp", "seq"), "mp"),
            P(("dp", "seq"), "mp"),
            P("mp", ("dp", "seq")),
            P(("dp", "seq"), "mp"),
            P(("dp", "seq"), "mp"),
            P("mp", ("dp", "seq")),
            P(),
            P(),
            P(None, "dp"),
            P(None, "dp", None),
        ),
        out_specs=(
            P(None, "dp", "seq", None),
            P(None, "dp", "seq", None),
            P(None, None, ("dp", "seq", "mp")),
            P(None, None, ("dp", "seq", "mp")),
        ),
        check_vma=False,
    )
```
